32 devices in a mesh: heads: 2 (over x), seq: 16 (over z, y, core).
Axes of the slice: x: 2, y: 2, z: 4, core: 2. Of those that a mesh axis runs over, the one named last changes fastest.
Arguments:
- q_nope: bfloat16 [1152, 64, 128], P('seq', 'heads'), may hold values from -6 to 6
- q_rope: bfloat16 [1152, 64, 64], P('seq', 'heads'), may hold values from -125 to 125
- latent: bfloat16 [1152, 512], P('seq'), may hold values from -6 to 6
- key_rope: bfloat16 [1152, 64], P('seq'), may hold values from -5 to 5
- absorb_key: bfloat16 [64, 128, 512], P('heads'), may hold values from -0.5 to 0.5
- absorb_value: bfloat16 [64, 512, 128], P('heads'), may hold values from -0.25 to 0.25
- w_out: bfloat16 [8192, 3584], P('heads', 'seq'), may hold values from -0.125 to 0.125
- residual: bfloat16 [1152, 3584], P(('seq', 'heads')), may hold values from -2 to 2
- norm_gain: float32 [3584], replicated, may hold values from 0.25 to 1.75
- span_table: int32 [32], replicated, may hold values from 0 to 31, each once
Outputs:
- new_residual: bfloat16 [1152, 3584], P(('seq', 'heads'))
- normed: bfloat16 [1152, 3584], P(('seq', 'heads'))
The draws below stay inside these ranges and needn't reach their ends.
Inputs may be any that keep to these rules, and one draw needn't show every extreme that they name: `span_table`: A permutation of the span numbers.
All inputs are finite; a program needn't handle non-finite values.
Results may differ from the reference program's by a relative error of at most 0.014.
Values may be sent and summed in bfloat16 or wider, within the bound.
No kernel may reach another device: no remote copies, remote signals or barrier semaphores. Data moves between devices by JAX's collectives and lax.ppermute only.
A program may use at most 128 MiB of HBM per device.

```python
import jax
import jax.numpy as jnp
from jax import lax

HEAD_DIM = 128
LATENT = 512
ROPE = 64
HEADS = 64
DW = 3584
TOKENS = 1152
SPAN = 36
SPANS = 32
N_HEADS = 2


def rope_pair(key):
    keys_part = jnp.clip(jax.random.normal(jax.random.fold_in(key, 11), (TOKENS, ROPE), jnp.float32), -5.0, 5.0)
    query_part = jnp.clip(jax.random.normal(jax.random.fold_in(key, 12), (TOKENS, HEADS, ROPE), jnp.float32), -5.0, 5.0)
    return (query_part, keys_part)


def draw_q_rope(key, part):
    return rope_pair(key)[0].astype(jnp.bfloat16)


def draw_key_rope(key, part):
    return rope_pair(key)[1].astype(jnp.bfloat16)


def block_levels(key, shape, split, low, top_value):
    gain = 1.0
    for dim, parts in split:
        steps = jax.random.uniform(jax.random.fold_in(jax.random.fold_in(key, 6), dim), (parts,), jnp.float32, low / len(split), top_value / len(split))
        gain = gain * jnp.repeat(jnp.exp(steps), shape[dim] // parts).reshape((-1,) + (1,) * (len(shape) - 1 - dim))
    return gain


def scatter_about(key, extent, deviation, reach, split=(), kind=jnp.bfloat16):
    level = block_levels(key, extent, split, -0.22, 0.18) if split else 1.0
    entries = jax.random.normal(key, extent, jnp.float32) * deviation * level
    return jnp.minimum(jnp.maximum(entries, -reach), reach).astype(kind)


def setup_inputs(seed: int = 0) -> dict:
    streams_of = jax.random.split(jax.random.key(seed), 11)
    return {
        "q_nope": scatter_about(streams_of[0], (TOKENS, HEADS, HEAD_DIM), 1.0, 6.0, ((0, 16), (1, 2))),
        "q_rope": draw_q_rope(jax.random.fold_in(streams_of[10], 71), 0),
        "latent": scatter_about(streams_of[2], (TOKENS, LATENT), 1.0, 6.0, ((0, 16),)),
        "key_rope": draw_key_rope(jax.random.fold_in(streams_of[10], 71), 0),
        "absorb_key": scatter_about(streams_of[4], (HEADS, HEAD_DIM, LATENT), HEAD_DIM ** -0.5, 0.5, ((0, 2),)),
        "absorb_value": scatter_about(streams_of[5], (HEADS, LATENT, HEAD_DIM), LATENT ** -0.5, 0.25, ((0, 2),)),
        "w_out": scatter_about(streams_of[6], (HEADS * HEAD_DIM, DW), (HEADS * HEAD_DIM // 4) ** -0.5, 0.125, ((0, 2), (1, 16))),
        "residual": scatter_about(streams_of[7], (TOKENS, DW), 0.3, 2.0, ((0, 32),)),
        "norm_gain": jnp.clip(1.0 + 0.15 * jax.random.normal(streams_of[8], (DW,), jnp.float32), 0.25, 1.75),
        "span_table": jax.random.permutation(streams_of[9], SPANS).astype(jnp.int32),
    }


score_scale = 192.0 ** (-0.5)

def reference(q_nope, q_rope, latent, key_rope, absorb_key, absorb_value, w_out, residual, norm_gain, span_table):
    index = jnp.arange(TOKENS, dtype=jnp.int32)
    pos = span_table[index // SPAN] * SPAN + index % SPAN
    visible = pos[None, :] <= pos[:, None]

    def one_head(pieces):
        query, rotary, w_key, w_value = pieces
        q_lat = jnp.dot(query, w_key, preferred_element_type=jnp.float32).astype(jnp.bfloat16)
        score = jnp.dot(q_lat, latent.T, preferred_element_type=jnp.float32)
        score = (score + jnp.dot(rotary, key_rope.T, preferred_element_type=jnp.float32)) * score_scale
        score = jnp.where(visible, score, jnp.float32(-1e+30))
        top = lax.optimization_barrier(jnp.max(score, axis=1, keepdims=True))
        weight = jnp.where(visible, jnp.exp(score - top), jnp.float32(0.0))
        total = lax.optimization_barrier(jnp.sum(weight, axis=1, keepdims=True))
        context = jnp.dot(weight.astype(jnp.bfloat16), latent, preferred_element_type=jnp.float32) / total
        return jnp.dot(context.astype(jnp.bfloat16), w_value, preferred_element_type=jnp.float32).astype(jnp.bfloat16)
    stacked = lax.map(one_head, (jnp.moveaxis(q_nope, 1, 0), jnp.moveaxis(q_rope, 1, 0), absorb_key, absorb_value))
    heads_out = jnp.moveaxis(stacked, 0, 1).reshape(TOKENS, HEADS * HEAD_DIM)
    group = HEADS * HEAD_DIM // N_HEADS
    summed = jnp.zeros((TOKENS, DW), jnp.float32)
    for member in range(N_HEADS):
        partial_value = jnp.dot(heads_out[:, member * group:(member + 1) * group], w_out[member * group:(member + 1) * group], preferred_element_type=jnp.float32)
        rounded = lax.optimization_barrier(partial_value.astype(jnp.bfloat16))
        summed = summed + rounded.astype(jnp.float32)
    hidden = residual.astype(jnp.float32) + summed
    new_residual = hidden.astype(jnp.bfloat16)
    scale = lax.rsqrt(lax.optimization_barrier(jnp.mean(hidden * hidden, axis=1, keepdims=True)) + 1e-06)
    normed = (hidden * scale * norm_gain.astype(jnp.float32)[None, :]).astype(jnp.bfloat16)
    return (new_residual, normed)
```

```python
import jax
import jax.numpy as jnp
from jax import lax
from jax.experimental import pallas as pl
from jax.experimental.pallas import tpu as pltpu
from jax.sharding import PartitionSpec as P

score_scale = 192.0 ** (-0.5)
LOG2E = 1.4426950408889634
LANES = 128


def positions(blocks, block_rows, span_len, span_table):
    per = block_rows // span_len
    spans = (blocks[:, None] * per + jnp.arange(per, dtype=jnp.int32)[None, :]).reshape(-1)
    picked = jnp.where(
        spans[:, None] == jnp.arange(span_table.shape[0], dtype=jnp.int32)[None, :],
        span_table[None, :],
        0,
    )
    first = jnp.sum(picked, axis=1) * span_len
    return (first[:, None] + jnp.arange(span_len, dtype=jnp.int32)[None, :]).reshape(-1)


def attend_kernel(off_ref, q_ref, kv_ref, qpos_ref, kpos_ref, wv_ref, out_ref, bias_ref):
    heads, rows, depth = q_ref.shape
    width = wv_ref.shape[1]
    keys = kv_ref.shape[0]

    @pl.when(pl.program_id(0) == 0)
    def _():
        bias_ref[...] = jnp.where(
            kpos_ref[...] <= qpos_ref[...], jnp.float32(0.0), jnp.float32(-1e30)
        )

    q = q_ref[...].reshape(heads * rows, depth)
    score = lax.dot_general(
        q, kv_ref[...], (((1,), (1,)), ((), ())), preferred_element_type=jnp.float32
    )
    score = score.reshape(heads, rows, keys) * (score_scale * LOG2E) + bias_ref[...][None]
    top = jnp.max(score, axis=2, keepdims=True)
    weight = jnp.exp2(score - top)
    total = jnp.sum(weight, axis=2, keepdims=True)
    context = jnp.dot(
        weight.astype(jnp.bfloat16).reshape(heads * rows, keys),
        kv_ref[:, :width],
        preferred_element_type=jnp.float32,
    ).reshape(heads, rows, width)
    context = (context / total).astype(jnp.bfloat16)
    for h in range(heads):
        part = jnp.dot(context[h], wv_ref[h], preferred_element_type=jnp.float32)
        out_ref[:, h * part.shape[1] : (h + 1) * part.shape[1]] = part.astype(out_ref.dtype)


def attend(offset, q, kv, qpos, kpos, wv, heads):
    total_heads, rows, depth = q.shape
    keys = kv.shape[0]
    width, size = wv.shape[1:]
    steps = total_heads // heads
    return pl.pallas_call(
        attend_kernel,
        grid_spec=pltpu.PrefetchScalarGridSpec(
            num_scalar_prefetch=1,
            grid=(steps,),
            in_specs=[
                pl.BlockSpec((heads, rows, depth), lambda i, off: (i, 0, 0)),
                pl.BlockSpec((keys, depth), lambda i, off: (0, 0)),
                pl.BlockSpec((rows, 1), lambda i, off: (0, 0)),
                pl.BlockSpec((1, keys), lambda i, off: (0, 0)),
                pl.BlockSpec((heads, width, size), lambda i, off: (off[0] * steps + i, 0, 0)),
            ],
            out_specs=pl.BlockSpec((rows, heads * size), lambda i, off: (0, i)),
            scratch_shapes=[pltpu.VMEM((rows, keys), jnp.float32)],
        ),
        out_shape=jax.ShapeDtypeStruct((rows, total_heads * size), jnp.bfloat16),
        compiler_params=pltpu.CompilerParams(vmem_limit_bytes=56 * 1024 * 1024),
        cost_estimate=pl.CostEstimate(
            flops=2 * total_heads * rows * keys * (depth + width),
            bytes_accessed=total_heads * (rows * depth + width * size) * 2,
            transcendentals=total_heads * rows * keys,
        ),
        name="attend",
    )(offset, q, kv, qpos, kpos, wv)


def per_device(
    q_nope, q_rope, latent, key_rope, absorb_key, absorb_value, w_out, residual, norm_gain, span_table
):
    tok, heads, size = q_nope.shape
    n_seq, n_heads = lax.axis_size("seq"), lax.axis_size("heads")
    depth_z = n_seq // 4
    span_len = tok * n_seq // span_table.shape[0]
    me = lax.axis_index("seq")
    core, row, slab = me % 2, (me // 2) % 2, me // 4
    half = heads // 2

    def swap(x, bit):
        return lax.ppermute(x, "seq", [(i, i ^ bit) for i in range(n_seq)])

    def shift(x, k):
        return lax.ppermute(x, "seq", [(i, (i + 4 * k) % n_seq) for i in range(n_seq)])

    pad = (-(latent.shape[1] + key_rope.shape[1])) % LANES
    kv_own = jnp.concatenate([latent, key_rope, jnp.zeros((tok, pad), latent.dtype)], axis=1)
    along = jnp.concatenate([kv_own] + [shift(kv_own, k) for k in range(1, depth_z)], axis=0)
    both = jnp.concatenate([along, swap(along, 2)], axis=0)
    kv = jnp.concatenate([both, swap(both, 1)], axis=0)
    ks = jnp.arange(depth_z, dtype=jnp.int32)
    source = (((slab - ks) % depth_z) * 4)[None, None, :]
    rows2 = (row ^ jnp.arange(2, dtype=jnp.int32))[None, :, None]
    cores2 = (core ^ jnp.arange(2, dtype=jnp.int32))[:, None, None]
    blocks = (source + rows2 * 2 + cores2).reshape(-1)
    kpos = positions(blocks, tok, span_len, span_table)[None, :]
    qpos = positions(me ^ jnp.arange(2, dtype=jnp.int32), tok, span_len, span_table)[:, None]

    def split_heads(q):
        mine = lax.dynamic_slice_in_dim(q, core * half, half, 1)
        theirs = lax.dynamic_slice_in_dim(q, (1 - core) * half, half, 1)
        return jnp.concatenate([mine, swap(theirs, 1)], axis=0)

    nope, rope = split_heads(q_nope), split_heads(q_rope)
    wk = lax.dynamic_slice_in_dim(absorb_key, core * half, half, 0)
    q_lat = jnp.einsum("thd,hdl->htl", nope, wk, preferred_element_type=jnp.float32)
    q_all = jnp.concatenate(
        [
            q_lat.astype(jnp.bfloat16),
            jnp.transpose(rope, (1, 0, 2)),
            jnp.zeros((half, 2 * tok, pad), jnp.bfloat16),
        ],
        axis=2,
    )

    w_t = w_out.T
    cols = w_t.shape[0]
    rows_half = half * size
    w_mine = lax.dynamic_slice_in_dim(w_t, core * rows_half, rows_half, 1)
    w_theirs = lax.dynamic_slice_in_dim(w_t, (1 - core) * rows_half, rows_half, 1)
    w_swapped = swap(w_theirs, 1)
    w_pair = jnp.zeros((2, cols, rows_half), w_t.dtype)
    w_pair = lax.dynamic_update_index_in_dim(w_pair, w_mine, core, 0)
    w_pair = lax.dynamic_update_index_in_dim(w_pair, w_swapped, 1 - core, 0)
    w_other = swap(w_pair, 2)
    w_all = jnp.zeros((2, 2, cols, rows_half), w_t.dtype)
    w_all = lax.dynamic_update_index_in_dim(w_all, w_pair, row, 0)
    w_all = lax.dynamic_update_index_in_dim(w_all, w_other, 1 - row, 0)
    w_all = w_all.reshape(4 * cols, rows_half)

    step_heads = max(h for h in (4, 2, 1) if half % h == 0 and h * tok * 2 * kv.shape[0] <= 1 << 20)
    mixed = attend(core.reshape(1), q_all, kv, qpos, kpos, absorb_value, step_heads)

    gathered = jnp.stack([mixed] + [shift(mixed, k) for k in range(1, depth_z)])
    partial = jnp.einsum("zti,oi->zto", gathered, w_all, preferred_element_type=jnp.float32)
    summed = partial[:, :tok] + swap(partial[:, tok:].astype(jnp.bfloat16), 1).astype(jnp.float32)
    if n_heads == 2:
        mine_x = lax.axis_index("heads")
        pieces = summed.reshape(depth_z, 2, tok // 2, 4 * cols)
        keep = lax.dynamic_index_in_dim(pieces, mine_x, 1, keepdims=False)
        send = lax.dynamic_index_in_dim(pieces, 1 - mine_x, 1, keepdims=False)
        got = lax.ppermute(send.astype(jnp.bfloat16), "heads", [(0, 1), (1, 0)])
        reduced = keep + got.astype(jnp.float32)
    else:
        reduced = lax.psum_scatter(
            summed.astype(jnp.bfloat16), "heads", scatter_dimension=1, tiled=True
        ).astype(jnp.float32)
    reduced = reduced.astype(jnp.bfloat16)
    projected = jnp.zeros((reduced.shape[1], depth_z, 4 * cols), jnp.bfloat16)
    for k in range(depth_z):
        piece = reduced[k] if k == 0 else shift(reduced[k], -k)
        projected = lax.dynamic_update_index_in_dim(projected, piece, (slab + k) % depth_z, 1)
    projected = projected.reshape(reduced.shape[1], depth_z * 4 * cols).astype(jnp.float32)
    hidden = residual.astype(jnp.float32) + projected
    new_residual = hidden.astype(jnp.bfloat16)
    scale = lax.rsqrt(jnp.mean(hidden * hidden, axis=1, keepdims=True) + 1e-06)
    normed = (hidden * scale * norm_gain[None, :]).astype(jnp.bfloat16)
    return (new_residual, normed)


def solution(mesh):
    in_specs = (
        P("seq", "heads", None),
        P("seq", "heads", None),
        P("seq", None),
        P("seq", None),
        P("heads", None, None),
        P("heads", None, None),
        P("heads", "seq"),
        P(("seq", "heads"), None),
        P(),
        P(),
    )
    out_specs = (P(("seq", "heads"), None), P(("seq", "heads"), None))
    return jax.shard_map(
        per_device, mesh=mesh, in_specs=in_specs, out_specs=out_specs, check_vma=False
    )
```

```python
import jax
import jax.numpy as jnp
from jax import lax
from jax.experimental import pallas as pl
from jax.experimental.pallas import tpu as pltpu
from jax.sharding import PartitionSpec as P

score_scale = 192.0 ** (-0.5)
LOG2E = 1.4426950408889634


def pack_kernel(lat_ref, rope_ref, out_ref):
    width = lat_ref.shape[1]
    out_ref[:, :width] = lat_ref[...]
    rope = rope_ref[...].astype(jnp.float32).T
    both = jnp.concatenate([rope, rope], axis=1)
    out_ref[:, width:] = both.astype(out_ref.dtype)


def pack(latent, rope_t):
    return pl.pallas_call(
        pack_kernel,
        out_shape=jax.ShapeDtypeStruct(
            (latent.shape[0], latent.shape[1] + 2 * rope_t.shape[0]), latent.dtype
        ),
        name="pack",
    )(latent, rope_t)


def attend_kernel(
    me_ref,
    table_ref,
    nope0_ref,
    nope1_ref,
    rope0_ref,
    rope1_ref,
    *refs,
):
    parts = refs[:4]
    wk_ref, wv_ref, out_ref, kv_ref, bias_ref, q_ref, sem = refs[4:]
    heads, tok, _ = nope0_ref.shape
    rows, keys = bias_ref.shape
    width = wk_ref.shape[2]
    rope = rope0_ref.shape[0] // heads
    span_len = keys // table_ref.shape[0]
    per = tok // span_len

    @pl.when(pl.program_id(0) == 0)
    def _():
        length = keys // 4
        copies = [
            pltpu.make_async_copy(part, kv_ref.at[pl.ds(n * length, length)], sem.at[n])
            for n, part in enumerate(parts)
        ]
        for copy in copies:
            copy.start()
        me = me_ref[0]
        slabs = length // tok
        lane = lax.broadcasted_iota(jnp.int32, (1, keys), 1)
        kpos = jnp.zeros((1, keys), jnp.int32)
        for n in range(keys // span_len):
            block, inside = n // per, n % per
            part, k = block // slabs, block % slabs
            slab = lax.rem((me >> 2) + (slabs - k), slabs)
            source = slab * 4 + ((me & 3) ^ ((part & 1) * 2 + (part >> 1)))
            first = table_ref[source * per + inside] * span_len - n * span_len
            kpos = jnp.where(lane >= n * span_len, first + lane, kpos)
        sub = lax.broadcasted_iota(jnp.int32, (rows, 1), 0)
        qpos = jnp.zeros((rows, 1), jnp.int32)
        for n in range(rows // span_len):
            source = me ^ (n // per)
            first = table_ref[source * per + n % per] * span_len - n * span_len
            qpos = jnp.where(sub >= n * span_len, first + sub, qpos)
        bias_ref[...] = jnp.where(kpos <= qpos, jnp.float32(0.0), jnp.float32(-1e30))
        for copy in copies:
            copy.wait()

    f32, bf16 = jnp.float32, jnp.bfloat16
    for h in range(heads):
        nope = jnp.concatenate([nope0_ref[h].astype(f32), nope1_ref[h].astype(f32)], axis=0)
        q_lat = jnp.dot(nope.astype(bf16), wk_ref[h], preferred_element_type=f32)
        q_ref[h * rows : (h + 1) * rows, :width] = q_lat.astype(bf16)
    lane = lax.broadcasted_iota(jnp.int32, (rows, 2 * rope), 1)
    for h in range(0, heads, 2):
        pick = slice(h * rope, (h + 2) * rope)
        pair = jnp.concatenate(
            [rope0_ref[pick, :].astype(f32).T, rope1_ref[pick, :].astype(f32).T], axis=0
        )
        q_ref[h * rows : (h + 1) * rows, width:] = jnp.where(lane < rope, pair, 0.0).astype(bf16)
        q_ref[(h + 1) * rows : (h + 2) * rows, width:] = jnp.where(lane < rope, 0.0, pair).astype(
            bf16
        )
    score = lax.dot_general(
        q_ref[...], kv_ref[...], (((1,), (1,)), ((), ())), preferred_element_type=f32
    )
    score = score.reshape(heads, rows, keys) * (score_scale * LOG2E) + bias_ref[...][None]
    top = jnp.max(score, axis=2, keepdims=True)
    weight = jnp.exp2(score - top)
    total = jnp.sum(weight, axis=2, keepdims=True)
    context = jnp.dot(
        weight.astype(bf16).reshape(heads * rows, keys),
        kv_ref[:, :width],
        preferred_element_type=f32,
    ).reshape(heads, rows, width)
    context = (context / total).astype(bf16)
    for h in range(heads):
        part = jnp.dot(context[h], wv_ref[h], preferred_element_type=f32)
        out_ref[:, h * part.shape[1] : (h + 1) * part.shape[1]] = part.astype(out_ref.dtype)


def attend(me, table, nope, rope, parts, wk, wv, group, groups, heads):
    half, tok, size = nope[0].shape
    steps = half // groups // heads
    rows = 2 * tok
    keys, depth = 4 * parts[0].shape[0], parts[0].shape[1]
    width = wk.shape[2]
    rope_rows = rope[0].shape[0] // half * heads
    first = group * steps

    def mine(i, me_ref, table_ref):
        return (first + i, 0, 0)

    def mine_flat(i, me_ref, table_ref):
        return (first + i, 0)

    def weight(i, me_ref, table_ref):
        return ((me_ref[0] & 1) * (half // heads) + first + i, 0, 0)

    return pl.pallas_call(
        attend_kernel,
        grid_spec=pltpu.PrefetchScalarGridSpec(
            num_scalar_prefetch=2,
            grid=(steps,),
            in_specs=[
                pl.BlockSpec((heads, tok, size), mine),
                pl.BlockSpec((heads, tok, size), mine),
                pl.BlockSpec((rope_rows, tok), mine_flat),
                pl.BlockSpec((rope_rows, tok), mine_flat),
                *[pl.BlockSpec(memory_space=pl.ANY)] * 4,
                pl.BlockSpec((heads, size, width), weight),
                pl.BlockSpec((heads, width, size), weight),
            ],
            out_specs=pl.BlockSpec((rows, heads * size), lambda i, me_ref, table_ref: (0, i)),
            scratch_shapes=[
                pltpu.VMEM((keys, depth), jnp.bfloat16),
                pltpu.VMEM((rows, keys), jnp.float32),
                pltpu.VMEM((heads * rows, depth), jnp.bfloat16),
                pltpu.SemaphoreType.DMA((4,)),
            ],
        ),
        out_shape=jax.ShapeDtypeStruct((rows, half // groups * size), jnp.bfloat16),
        compiler_params=pltpu.CompilerParams(vmem_limit_bytes=32 * 1024 * 1024),
        cost_estimate=pl.CostEstimate(
            flops=2 * half // groups * rows * keys * (depth + width),
            bytes_accessed=half // groups * (rows + 2 * width) * size * 2,
            transcendentals=half // groups * rows * keys,
        ),
        name="attend",
    )(me, table, *nope, *rope, *parts, wk, wv)


def finish_kernel(me_ref, res_ref, gain_ref, *refs):
    pieces = refs[:-3]
    new_ref, normed_ref, hidden_ref = refs[-3:]
    me = me_ref[0]
    cols = pieces[0].shape[2]
    wide = 4 * cols
    for k, piece in enumerate(pieces):
        at = pl.multiple_of(me_ref[1 + k] * wide, wide)
        for case in range(4):

            @pl.when((me & 3) == case)
            def _():
                row = jnp.concatenate([piece[j ^ case] for j in range(4)], axis=1)
                old = res_ref[:, pl.ds(at, wide)].astype(jnp.float32)
                hidden_ref[:, pl.ds(at, wide)] = old + row.astype(jnp.float32)

    hidden = hidden_ref[...]
    new_ref[...] = hidden.astype(new_ref.dtype)
    scale = lax.rsqrt(jnp.mean(hidden * hidden, axis=1, keepdims=True) + 1e-06)
    normed_ref[...] = (hidden * scale * gain_ref[...]).astype(normed_ref.dtype)


def finish(places, residual, gain, pieces):
    vmem = pl.BlockSpec(memory_space=pltpu.VMEM)
    out = jax.ShapeDtypeStruct(residual.shape, jnp.bfloat16)
    return pl.pallas_call(
        finish_kernel,
        in_specs=[pl.BlockSpec(memory_space=pltpu.SMEM)] + [vmem] * (2 + len(pieces)),
        out_specs=[vmem, vmem],
        out_shape=[out, out],
        scratch_shapes=[pltpu.VMEM(residual.shape, jnp.float32)],
        name="finish",
    )(places, residual, gain, *pieces)


def per_device(
    q_nope, q_rope, latent, key_rope, absorb_key, absorb_value, w_out, residual, norm_gain, span_table
):
    f32, bf16 = jnp.float32, jnp.bfloat16
    tok, heads, size = q_nope.shape
    rope = q_rope.shape[2]
    n_seq, n_heads = lax.axis_size("seq"), lax.axis_size("heads")
    depth_z = n_seq // 4
    me = lax.axis_index("seq").astype(jnp.int32)
    core, slab = me & 1, me >> 2
    half = heads // 2

    def swap(x, bit):
        return lax.ppermute(x, "seq", [(i, i ^ bit) for i in range(n_seq)])

    def shift(x, k):
        return lax.ppermute(x, "seq", [(i, (i + 4 * k) % n_seq) for i in range(n_seq)])

    def move(x, pairs):
        return lax.ppermute(x, "seq", [(4 * a + r, 4 * b + r) for a, b in pairs for r in range(4)])

    kv_own = pack(latent, key_rope.T)
    zs = [kv_own] + [shift(kv_own, k) for k in range(1, depth_z)]
    ys = [swap(b, 2) for b in zs]
    along, across = jnp.concatenate(zs, axis=0), jnp.concatenate(ys, axis=0)
    parts = [along, across, swap(along, 1), swap(across, 1)]

    def split_heads(x, count):
        mine = lax.dynamic_slice_in_dim(x, core * count, count, 0)
        return mine, swap(lax.dynamic_slice_in_dim(x, (1 - core) * count, count, 0), 1)

    nope = split_heads(jnp.transpose(q_nope, (1, 0, 2)), half)
    rotary = split_heads(jnp.transpose(q_rope, (1, 2, 0)).reshape(heads * rope, tok), half * rope)

    w_t = w_out.T
    cols = w_t.shape[0]
    span = half * size
    w_mine = lax.dynamic_slice_in_dim(w_t, core * span, span, 1)
    w_core = swap(lax.dynamic_slice_in_dim(w_t, (1 - core) * span, span, 1), 1)
    w_mine, w_core, across_done = lax.optimization_barrier((w_mine, w_core, ys[-1]))
    w_all = jnp.stack([w_mine, w_core, swap(w_mine, 2), swap(w_core, 2)])

    groups = 2
    step_heads = max(
        h for h in (4, 2) if half // groups % h == 0 and h * tok * 8 * tok * depth_z <= 3 << 19
    )
    line = depth_z == 4
    inner = (slab == 1) | (slab == 2)
    blocks = []
    for g in range(groups):
        mixed = attend(
            me.reshape(1), span_table, nope, rotary, parts, absorb_key, absorb_value, g, groups, step_heads
        )
        if line:
            near = move(mixed, [(0, 1), (1, 0), (2, 3), (3, 2)])
            mid = move(mixed, [(1, 2), (2, 1)])
            out2 = move(mid, [(1, 0), (2, 3)])
            far = move(near, [(1, 2), (2, 1)])
            out3 = move(far, [(1, 0), (2, 3)])
            blocks.append([mixed, near, jnp.where(inner, mid, out2), jnp.where(inner, far, out3)])
        else:
            blocks.append([mixed] + [shift(mixed, k) for k in range(1, depth_z)])

    def project(some):
        total = 0.0
        for g in range(groups):
            rows = jnp.stack([blocks[g][b] for b in some])
            lo, hi = g * span // groups, (g + 1) * span // groups
            total = total + jnp.einsum(
                "zti,joi->jzto", rows, w_all[:, :, lo:hi], preferred_element_type=f32
            )
        other = swap(total[:, :, tok:].astype(bf16), 1)
        total = total[:, :, :tok] + jnp.stack([other[j ^ 1] for j in range(4)]).astype(f32)
        if n_heads == 2:
            x = lax.axis_index("heads")
            total = total.reshape(4, len(some), 2, tok // 2, cols)
            keep = lax.dynamic_index_in_dim(total, x, 2, keepdims=False)
            send = lax.dynamic_index_in_dim(total, 1 - x, 2, keepdims=False)
            got = lax.ppermute(send.astype(bf16), "heads", [(0, 1), (1, 0)])
            total = keep + got.astype(f32)
        else:
            total = lax.psum_scatter(
                total.astype(bf16), "heads", scatter_dimension=2, tiled=True
            )
        total = total.astype(bf16)
        return [total[:, n] for n in range(len(some))]

    if line:
        early = project([0, 1, 2])
        (late,) = project([3])
        got1 = move(early[1], [(0, 1), (1, 0), (2, 3), (3, 2)])
        in2, in3 = move(early[2], [(0, 2), (3, 1)]), move(early[2], [(1, 2), (2, 1)])
        end2, end3 = move(late, [(1, 3), (2, 0)]), move(late, [(0, 3), (3, 0)])
        pieces = [early[0], got1, jnp.where(inner, in2, end2), jnp.where(inner, in3, end3)]
        places = slab ^ jnp.arange(4, dtype=jnp.int32)
    else:
        mine = project(list(range(depth_z)))
        pieces = [mine[0]] + [shift(mine[k], -k) for k in range(1, depth_z)]
        places = lax.rem(slab + jnp.arange(depth_z, dtype=jnp.int32), depth_z)
    if 4 * cols % 128 == 0:
        places = jnp.concatenate([me.reshape(1), places])
        return tuple(finish(places, residual, norm_gain[None, :], pieces))
    order = jnp.arange(depth_z, dtype=jnp.int32)
    order = jnp.sum(jnp.where(places[None, :] == order[:, None], order[None, :], 0), axis=1)
    columns = jnp.take(jnp.stack(pieces), order, axis=0)
    columns = jnp.take(columns, jnp.arange(4, dtype=jnp.int32) ^ (me & 3), axis=1)
    hidden = residual.astype(f32) + jnp.moveaxis(columns, 2, 0).reshape(residual.shape).astype(f32)
    scale = lax.rsqrt(jnp.mean(hidden * hidden, axis=1, keepdims=True) + 1e-06)
    return (hidden.astype(bf16), (hidden * scale * norm_gain[None, :]).astype(bf16))


def solution(mesh):
    in_specs = (
        P("seq", "heads", None),
        P("seq", "heads", None),
        P("seq", None),
        P("seq", None),
        P("heads", None, None),
        P("heads", None, None),
        P("heads", "seq"),
        P(("seq", "heads"), None),
        P(),
        P(),
    )
    out_specs = (P(("seq", "heads"), None), P(("seq", "heads"), None))
    return jax.shard_map(
        per_device, mesh=mesh, in_specs=in_specs, out_specs=out_specs, check_vma=False
    )
```

```python
import functools

import jax
import jax.numpy as jnp
from jax import lax
from jax.experimental import pallas as pl
from jax.experimental.pallas import tpu as pltpu
from jax.sharding import PartitionSpec as P

score_scale = 192.0 ** (-0.5)
LOG2E = 1.4426950408889634


def pack_kernel(lat_ref, rope_ref, out_ref):
    width = lat_ref.shape[1]
    out_ref[:, :width] = lat_ref[...]
    rope = rope_ref[...].astype(jnp.float32).T
    both = jnp.concatenate([rope, rope], axis=1)
    out_ref[:, width:] = both.astype(out_ref.dtype)


def pack(latent, rope_t):
    return pl.pallas_call(
        pack_kernel,
        out_shape=jax.ShapeDtypeStruct(
            (latent.shape[0], latent.shape[1] + 2 * rope_t.shape[0]), latent.dtype
        ),
        compiler_params=pltpu.CompilerParams(vmem_limit_bytes=8 * 1024 * 1024),
        name="pack",
    )(latent, rope_t)


def attend_kernel(
    me_ref,
    table_ref,
    nope0_ref,
    nope1_ref,
    rope0_ref,
    rope1_ref,
    *refs,
):
    parts = refs[:4]
    wk_ref, wv_ref, out_ref, kv_ref, bias_ref, q_ref, s_ref, p_ref, total_ref, sem = refs[4:]
    heads, tok, _ = nope0_ref.shape
    rows, keys = bias_ref.shape
    width = wk_ref.shape[2]
    rope = rope0_ref.shape[0] // heads
    span_len = keys // table_ref.shape[0]
    per = tok // span_len

    length = keys // 4
    copies = [
        pltpu.make_async_copy(part, kv_ref.at[pl.ds(n * length, length)], sem.at[n])
        for n, part in enumerate(parts)
    ]

    @pl.when(pl.program_id(0) == 0)
    def _():
        for copy in copies:
            copy.start()
        me = me_ref[0]
        slabs = length // tok
        lane = lax.broadcasted_iota(jnp.int32, (1, keys), 1)
        kpos = jnp.zeros((1, keys), jnp.int32)
        for n in range(keys // span_len):
            block, inside = n // per, n % per
            part, k = block // slabs, block % slabs
            slab = (me >> 2) ^ k
            source = slab * 4 + ((me & 3) ^ ((part & 1) * 2 + (part >> 1)))
            first = table_ref[source * per + inside] * span_len - n * span_len
            kpos = jnp.where(lane >= n * span_len, first + lane, kpos)
        sub = lax.broadcasted_iota(jnp.int32, (rows, 1), 0)
        qpos = jnp.zeros((rows, 1), jnp.int32)
        for n in range(rows // span_len):
            source = me ^ (n // per)
            first = table_ref[source * per + n % per] * span_len - n * span_len
            qpos = jnp.where(sub >= n * span_len, first + sub, qpos)
        bias_ref[...] = jnp.where(kpos <= qpos, jnp.float32(0.0), jnp.float32(-1e30))

    f32, bf16 = jnp.float32, jnp.bfloat16
    for h in range(heads):
        nope = jnp.concatenate([nope0_ref[h].astype(f32), nope1_ref[h].astype(f32)], axis=0)
        q_lat = jnp.dot(nope.astype(bf16), wk_ref[h], preferred_element_type=f32)
        q_ref[h * rows : (h + 1) * rows, :width] = q_lat.astype(bf16)
    lane = lax.broadcasted_iota(jnp.int32, (rows, 2 * rope), 1)
    for h in range(0, heads, 2):
        pick = slice(h * rope, (h + 2) * rope)
        pair = jnp.concatenate(
            [rope0_ref[pick, :].astype(f32).T, rope1_ref[pick, :].astype(f32).T], axis=0
        )
        q_ref[h * rows : (h + 1) * rows, width:] = jnp.where(lane < rope, pair, 0.0).astype(bf16)
        q_ref[(h + 1) * rows : (h + 2) * rows, width:] = jnp.where(lane < rope, 0.0, pair).astype(
            bf16
        )

    @pl.when(pl.program_id(0) == 0)
    def _():
        for copy in copies:
            copy.wait()

    units, step = 2, 16
    count = heads * rows // units

    def scores(u):
        s_ref[pl.ds(u * count, count), :] = lax.dot_general(
            q_ref[pl.ds(u * count, count), :],
            kv_ref[...],
            (((1,), (1,)), ((), ())),
            preferred_element_type=f32,
        )

    def weights(u):
        for r in range(u * count, (u + 1) * count, step):
            block = s_ref[r : r + step, :] * (score_scale * LOG2E)
            block = block + bias_ref[r % rows : r % rows + step, :]
            weight = jnp.exp2(block - jnp.max(block, axis=1, keepdims=True))
            total_ref[r : r + step, :] = 1.0 / jnp.sum(weight, axis=1, keepdims=True)
            p_ref[r : r + step, :] = weight.astype(bf16)

    def outputs(u):
        context = jnp.dot(
            p_ref[pl.ds(u * count, count), :], kv_ref[:, :width], preferred_element_type=f32
        )
        context = (context * total_ref[pl.ds(u * count, count), :]).astype(bf16)
        for n in range(count // rows):
            h = u * (count // rows) + n
            part = jnp.dot(
                context[n * rows : (n + 1) * rows], wv_ref[h], preferred_element_type=f32
            )
            out_ref[:, h * part.shape[1] : (h + 1) * part.shape[1]] = part.astype(out_ref.dtype)

    for u in range(units + 2):
        if u < units:
            scores(u)
        if 1 <= u <= units:
            weights(u - 1)
        if u >= 2:
            outputs(u - 2)


def attend(me, table, nope, rope, parts, wk, wv, group, groups, heads):
    half, tok, size = nope[0].shape
    steps = half // groups // heads
    rows = 2 * tok
    keys, depth = 4 * parts[0].shape[0], parts[0].shape[1]
    width = wk.shape[2]
    rope_rows = rope[0].shape[0] // half * heads
    first = group * steps

    def mine(i, me_ref, table_ref):
        return (first + i, 0, 0)

    def mine_flat(i, me_ref, table_ref):
        return (first + i, 0)

    return pl.pallas_call(
        attend_kernel,
        grid_spec=pltpu.PrefetchScalarGridSpec(
            num_scalar_prefetch=2,
            grid=(steps,),
            in_specs=[
                pl.BlockSpec((heads, tok, size), mine),
                pl.BlockSpec((heads, tok, size), mine),
                pl.BlockSpec((rope_rows, tok), mine_flat),
                pl.BlockSpec((rope_rows, tok), mine_flat),
                *[pl.BlockSpec(memory_space=pl.ANY)] * 4,
                pl.BlockSpec((heads, size, width), mine),
                pl.BlockSpec((heads, width, size), mine),
            ],
            out_specs=pl.BlockSpec((rows, heads * size), lambda i, me_ref, table_ref: (0, i)),
            scratch_shapes=[
                pltpu.VMEM((keys, depth), jnp.bfloat16),
                pltpu.VMEM((rows, keys), jnp.float32),
                pltpu.VMEM((heads * rows, depth), jnp.bfloat16),
                pltpu.VMEM((heads * rows, keys), jnp.float32),
                pltpu.VMEM((heads * rows, keys), jnp.bfloat16),
                pltpu.VMEM((heads * rows, 1), jnp.float32),
                pltpu.SemaphoreType.DMA((4,)),
            ],
        ),
        out_shape=jax.ShapeDtypeStruct((rows, half // groups * size), jnp.bfloat16),
        compiler_params=pltpu.CompilerParams(vmem_limit_bytes=24 * 1024 * 1024),
        cost_estimate=pl.CostEstimate(
            flops=2 * half // groups * rows * keys * (depth + width),
            bytes_accessed=half // groups * (rows + 2 * width) * size * 2,
            transcendentals=half // groups * rows * keys,
        ),
        name="attend",
    )(me, table, *nope, *rope, *parts, wk, wv)


def project_kernel(plain, choice, skip, prev, me_ref, *refs):
    refs = list(refs)

    def take(count):
        out, refs[:count] = refs[:count], []
        return out

    fixed = [take(2) for _ in range(plain)]
    options = [take(2) for _ in range(choice)]
    weights = take(len(refs) - 2 - (2 if prev else 0))
    before = take(2) if prev else []
    keep_ref, send_ref = refs
    tok = keep_ref.shape[2]
    for old, new in zip(before, refs):
        new[: old.shape[0], : old.shape[1]] = old[...]

    def emit(blocks, at, first):
        for j in range(first, len(weights)):
            total = 0.0
            for g in range(2):
                rows = jnp.concatenate([block[g][...] for block in blocks], axis=0)
                width = rows.shape[1]
                total = total + lax.dot_general(
                    rows,
                    weights[j][:, g * width : (g + 1) * width],
                    (((1,), (1,)), ((), ())),
                    preferred_element_type=jnp.float32,
                )
            for n in range(len(blocks)):
                start = 2 * tok * n
                keep_ref[j, at + n] = total[start : start + tok]
                send_ref[j, at + n] = total[start + tok : start + 2 * tok].astype(send_ref.dtype)

    if fixed:
        emit(fixed, 0, skip)
    slab = me_ref[0] >> 2
    inner = (slab == 1) | (slab == 2)
    for n, option in enumerate(options):

        @pl.when(inner if n == 0 else ~inner)
        def _():
            emit([option], plain, 0)


def project(me, fixed, options, weights, tok, skip=0, before=()):
    count = len(fixed) + bool(options)
    shape = (len(weights), count, tok, weights[0].shape[0])
    operands = [ref for block in [*fixed, *options] for ref in block] + list(weights) + list(before)
    vmem = pl.BlockSpec(memory_space=pltpu.VMEM)
    return pl.pallas_call(
        functools.partial(project_kernel, len(fixed), len(options), skip, bool(before)),
        in_specs=[pl.BlockSpec(memory_space=pltpu.SMEM)] + [vmem] * len(operands),
        out_specs=[vmem, vmem],
        out_shape=[
            jax.ShapeDtypeStruct(shape, jnp.float32),
            jax.ShapeDtypeStruct(shape, jnp.bfloat16),
        ],
        compiler_params=pltpu.CompilerParams(vmem_limit_bytes=16 * 1024 * 1024),
        cost_estimate=pl.CostEstimate(
            flops=4 * tok * count * sum(w.size for w in weights),
            bytes_accessed=0,
            transcendentals=0,
        ),
        name="project",
    )(me, *operands)


def finish_kernel(me_ref, res_ref, gain_ref, *refs):
    pieces = refs[:-3]
    new_ref, normed_ref, hidden_ref = refs[-3:]
    me = me_ref[0]
    cols = pieces[0].shape[2]
    wide = 4 * cols
    for k, piece in enumerate(pieces):
        at = pl.multiple_of(me_ref[1 + k] * wide, wide)
        for case in range(4):

            @pl.when((me & 3) == case)
            def _():
                row = jnp.concatenate([piece[j ^ case] for j in range(4)], axis=1)
                old = res_ref[:, pl.ds(at, wide)].astype(jnp.float32)
                hidden_ref[:, pl.ds(at, wide)] = old + row.astype(jnp.float32)

    hidden = hidden_ref[...]
    new_ref[...] = hidden.astype(new_ref.dtype)
    scale = lax.rsqrt(jnp.mean(hidden * hidden, axis=1, keepdims=True) + 1e-06)
    normed_ref[...] = (hidden * scale * gain_ref[...]).astype(normed_ref.dtype)


def finish(places, residual, gain, pieces):
    vmem = pl.BlockSpec(memory_space=pltpu.VMEM)
    out = jax.ShapeDtypeStruct(residual.shape, jnp.bfloat16)
    return pl.pallas_call(
        finish_kernel,
        in_specs=[pl.BlockSpec(memory_space=pltpu.SMEM)] + [vmem] * (2 + len(pieces)),
        out_specs=[vmem, vmem],
        out_shape=[out, out],
        scratch_shapes=[pltpu.VMEM(residual.shape, jnp.float32)],
        compiler_params=pltpu.CompilerParams(vmem_limit_bytes=8 * 1024 * 1024),
        name="finish",
    )(places, residual, gain, *pieces)


def per_device(
    q_nope, q_rope, latent, key_rope, absorb_key, absorb_value, w_out, residual, norm_gain, span_table
):
    f32, bf16 = jnp.float32, jnp.bfloat16
    tok, heads, size = q_nope.shape
    rope = q_rope.shape[2]
    n_seq, n_heads = lax.axis_size("seq"), lax.axis_size("heads")
    depth_z = n_seq // 4
    me = lax.axis_index("seq").astype(jnp.int32)
    core, slab = me & 1, me >> 2
    half = heads // 2

    line = depth_z == 4

    def swap(x, bit):
        return lax.ppermute(x, "seq", [(i, i ^ bit) for i in range(n_seq)])

    def move(x, pairs):
        return lax.ppermute(x, "seq", [(4 * a + r, 4 * b + r) for a, b in pairs for r in range(4)])

    kv_own = pack(latent, key_rope.T)
    zs, ys = [kv_own], [swap(kv_own, 2)]
    for k in range(1, depth_z):
        k = (k ^ (k >> 1)) if line else k
        zs.append(swap(kv_own, 4 * k))
        ys.append(swap(zs[-1], 2))
    if line:
        zs, ys = [zs[k] for k in (0, 1, 3, 2)], [ys[k] for k in (0, 1, 3, 2)]
    along, across = jnp.concatenate(zs, axis=0), jnp.concatenate(ys, axis=0)

    def split_heads(x, count):
        mine = lax.dynamic_slice_in_dim(x, core * count, count, 0)
        theirs = lax.dynamic_slice_in_dim(x, (1 - core) * count, count, 0)
        return mine, swap(theirs, 1)

    nope = split_heads(jnp.transpose(q_nope, (1, 0, 2)), half)
    rotary = split_heads(jnp.transpose(q_rope, (1, 2, 0)).reshape(heads * rope, tok), half * rope)

    wk = lax.dynamic_slice_in_dim(absorb_key, core * half, half, 0)
    wv = lax.dynamic_slice_in_dim(absorb_value, core * half, half, 0)
    along, wk, wv, *own = lax.optimization_barrier((along, wk, wv, nope[0], rotary[0]))
    nope, rotary = (own[0], nope[1]), (own[1], rotary[1])
    parts = [along, across, swap(along, 1), swap(across, 1)]

    w_t = w_out.T
    cols = w_t.shape[0]
    span = half * size
    w_mine = lax.dynamic_slice_in_dim(w_t, core * span, span, 1)
    w_theirs = lax.dynamic_slice_in_dim(w_t, (1 - core) * span, span, 1)
    w_core = swap(w_theirs, 1)
    weights = [w_mine, w_core, swap(w_mine, 2), swap(w_core, 2)]

    groups = 2
    step_heads = max(
        h for h in (4, 2) if half // groups % h == 0 and h * tok * 8 * tok * depth_z <= 3 << 19
    )
    blocks = []
    for g in range(groups):
        mixed = attend(
            me.reshape(1),
            span_table,
            nope,
            rotary,
            parts,
            wk,
            wv,
            g,
            groups,
            step_heads,
        )
        if line:
            near = move(mixed, [(0, 1), (1, 0), (2, 3), (3, 2)])
            mid = move(mixed, [(1, 2), (2, 1)])
            out2 = move(mid, [(1, 0), (2, 3)])
            far = move(near, [(1, 2), (2, 1)])
            out3 = move(far, [(1, 0), (2, 3)])
            blocks.append([mixed, near, far, out2, mid, out3])
        else:
            blocks.append([mixed] + [swap(mixed, 4 * k) for k in range(1, depth_z)])

    def reduce(keep, send):
        count = keep.shape[1]
        other = swap(send, 1)
        total = keep + jnp.stack([other[j ^ 1] for j in range(4)]).astype(f32)
        if n_heads == 2:
            x = lax.axis_index("heads")
            total = total.reshape(4, count, 2, tok // 2, cols)
            keep = lax.dynamic_index_in_dim(total, x, 2, keepdims=False)
            send = lax.dynamic_index_in_dim(total, 1 - x, 2, keepdims=False)
            got = lax.ppermute(send.astype(bf16), "heads", [(0, 1), (1, 0)])
            total = keep + got.astype(f32)
        else:
            total = lax.psum_scatter(total.astype(bf16), "heads", scatter_dimension=2, tiled=True)
        total = total.astype(bf16)
        return [total[:, n] for n in range(count)]

    if line:
        mixed, near, far, out2, mid, out3 = zip(*blocks)
        me1 = me.reshape(1)
        first = project(me1, [mixed, near], [], weights[:2], tok)
        early = project(me1, [mixed, near], [far, out2], weights, tok, 2, first)
        late = project(me1, [], [mid, out3], weights, tok)
        mine = reduce(*early) + reduce(*late)
    else:
        rows = jnp.stack([jnp.concatenate(parts, axis=1) for parts in zip(*blocks)])
        total = jnp.einsum("zti,joi->jzto", rows, jnp.stack(weights), preferred_element_type=f32)
        mine = reduce(total[:, :, :tok], total[:, :, tok:].astype(bf16))
    pieces = [mine[0]] + [swap(mine[k], 4 * k) for k in range(1, depth_z)]
    places = slab ^ jnp.arange(depth_z, dtype=jnp.int32)
    if 4 * cols % 128 == 0:
        places = jnp.concatenate([me.reshape(1), places])
        return tuple(finish(places, residual, norm_gain[None, :], pieces))
    order = jnp.arange(depth_z, dtype=jnp.int32)
    order = jnp.sum(jnp.where(places[None, :] == order[:, None], order[None, :], 0), axis=1)
    columns = jnp.take(jnp.stack(pieces), order, axis=0)
    columns = jnp.take(columns, jnp.arange(4, dtype=jnp.int32) ^ (me & 3), axis=1)
    hidden = residual.astype(f32) + jnp.moveaxis(columns, 2, 0).reshape(residual.shape).astype(f32)
    scale = lax.rsqrt(jnp.mean(hidden * hidden, axis=1, keepdims=True) + 1e-06)
    return (hidden.astype(bf16), (hidden * scale * norm_gain[None, :]).astype(bf16))


def solution(mesh):
    in_specs = (
        P("seq", "heads", None),
        P("seq", "heads", None),
        P("seq", None),
        P("seq", None),
        P("heads", None, None),
        P("heads", None, None),
        P("heads", "seq"),
        P(("seq", "heads"), None),
        P(),
        P(),
    )
    out_specs = (P(("seq", "heads"), None), P(("seq", "heads"), None))

    return jax.shard_map(
        per_device, mesh=mesh, in_specs=in_specs, out_specs=out_specs, check_vma=False
    )
```

```python
import functools

import jax
import jax.numpy as jnp
from jax import lax
from jax.experimental import pallas as pl
from jax.experimental.pallas import tpu as pltpu
from jax.sharding import PartitionSpec as P

score_scale = 192.0 ** (-0.5)
LOG2E = 1.4426950408889634


def pack_kernel(lat_ref, rope_ref, out_ref):
    width = lat_ref.shape[1]
    out_ref[:, :width] = lat_ref[...]
    rope = rope_ref[...].astype(jnp.float32).T
    both = jnp.concatenate([rope, rope], axis=1)
    out_ref[:, width:] = both.astype(out_ref.dtype)


def pack(latent, rope_t):
    return pl.pallas_call(
        pack_kernel,
        out_shape=jax.ShapeDtypeStruct(
            (latent.shape[0], latent.shape[1] + 2 * rope_t.shape[0]), latent.dtype
        ),
        compiler_params=pltpu.CompilerParams(vmem_limit_bytes=8 * 1024 * 1024),
        name="pack",
    )(latent, rope_t)


def attend_kernel(
    me_ref,
    table_ref,
    nope0_ref,
    nope1_ref,
    rope0_ref,
    rope1_ref,
    *refs,
):
    parts = refs[:4]
    wk_ref, wv_ref, out_ref, kv_ref, bias_ref, q_ref, s_ref, p_ref, total_ref, sem = refs[4:]
    heads, tok, _ = nope0_ref.shape
    rows, keys = bias_ref.shape
    width = wk_ref.shape[2]
    rope = rope0_ref.shape[0] // heads
    span_len = keys // table_ref.shape[0]
    per = tok // span_len

    length = keys // 4
    copies = [
        pltpu.make_async_copy(part, kv_ref.at[pl.ds(n * length, length)], sem.at[n])
        for n, part in enumerate(parts)
    ]

    @pl.when(pl.program_id(0) == 0)
    def _():
        for copy in copies:
            copy.start()
        me = me_ref[0]
        slabs = length // tok
        lane = lax.broadcasted_iota(jnp.int32, (1, keys), 1)
        kpos = jnp.zeros((1, keys), jnp.int32)
        for n in range(keys // span_len):
            block, inside = n // per, n % per
            part, k = block // slabs, block % slabs
            slab = (me >> 2) ^ k
            source = slab * 4 + ((me & 3) ^ ((part & 1) * 2 + (part >> 1)))
            first = table_ref[source * per + inside] * span_len - n * span_len
            kpos = jnp.where(lane >= n * span_len, first + lane, kpos)
        sub = lax.broadcasted_iota(jnp.int32, (rows, 1), 0)
        qpos = jnp.zeros((rows, 1), jnp.int32)
        for n in range(rows // span_len):
            source = me ^ (n // per)
            first = table_ref[source * per + n % per] * span_len - n * span_len
            qpos = jnp.where(sub >= n * span_len, first + sub, qpos)
        bias_ref[...] = jnp.where(kpos <= qpos, jnp.float32(0.0), jnp.float32(-1e30))

    f32, bf16 = jnp.float32, jnp.bfloat16
    for h in range(heads):
        nope = jnp.concatenate([nope0_ref[h].astype(f32), nope1_ref[h].astype(f32)], axis=0)
        q_lat = jnp.dot(nope.astype(bf16), wk_ref[h], preferred_element_type=f32)
        q_ref[h * rows : (h + 1) * rows, :width] = q_lat.astype(bf16)
    lane = lax.broadcasted_iota(jnp.int32, (rows, 2 * rope), 1)
    for h in range(0, heads, 2):
        pick = slice(h * rope, (h + 2) * rope)
        pair = jnp.concatenate(
            [rope0_ref[pick, :].astype(f32).T, rope1_ref[pick, :].astype(f32).T], axis=0
        )
        q_ref[h * rows : (h + 1) * rows, width:] = jnp.where(lane < rope, pair, 0.0).astype(bf16)
        q_ref[(h + 1) * rows : (h + 2) * rows, width:] = jnp.where(lane < rope, 0.0, pair).astype(
            bf16
        )

    @pl.when(pl.program_id(0) == 0)
    def _():
        for copy in copies:
            copy.wait()

    units, step = 2, 16
    count = heads * rows // units

    def scores(u):
        s_ref[pl.ds(u * count, count), :] = lax.dot_general(
            q_ref[pl.ds(u * count, count), :],
            kv_ref[...],
            (((1,), (1,)), ((), ())),
            preferred_element_type=f32,
        )

    def weights(u):
        for r in range(u * count, (u + 1) * count, step):
            block = s_ref[r : r + step, :] * (score_scale * LOG2E)
            block = block + bias_ref[r % rows : r % rows + step, :]
            weight = jnp.exp2(block - jnp.max(block, axis=1, keepdims=True))
            total_ref[r : r + step, :] = 1.0 / jnp.sum(weight, axis=1, keepdims=True)
            p_ref[r : r + step, :] = weight.astype(bf16)

    def outputs(u):
        context = jnp.dot(
            p_ref[pl.ds(u * count, count), :], kv_ref[:, :width], preferred_element_type=f32
        )
        context = (context * total_ref[pl.ds(u * count, count), :]).astype(bf16)
        for n in range(count // rows):
            h = u * (count // rows) + n
            part = jnp.dot(
                context[n * rows : (n + 1) * rows], wv_ref[h], preferred_element_type=f32
            )
            out_ref[:, h * part.shape[1] : (h + 1) * part.shape[1]] = part.astype(out_ref.dtype)

    for u in range(units + 2):
        if u < units:
            scores(u)
        if 1 <= u <= units:
            weights(u - 1)
        if u >= 2:
            outputs(u - 2)


def attend(me, table, nope, rope, parts, wk, wv, group, groups, heads):
    half, tok, size = nope[0].shape
    steps = half // groups // heads
    rows = 2 * tok
    keys, depth = 4 * parts[0].shape[0], parts[0].shape[1]
    width = wk.shape[2]
    rope_rows = rope[0].shape[0] // half * heads
    first = group * steps

    def mine(i, me_ref, table_ref):
        return (first + i, 0, 0)

    def mine_flat(i, me_ref, table_ref):
        return (first + i, 0)

    return pl.pallas_call(
        attend_kernel,
        grid_spec=pltpu.PrefetchScalarGridSpec(
            num_scalar_prefetch=2,
            grid=(steps,),
            in_specs=[
                pl.BlockSpec((heads, tok, size), mine),
                pl.BlockSpec((heads, tok, size), mine),
                pl.BlockSpec((rope_rows, tok), mine_flat),
                pl.BlockSpec((rope_rows, tok), mine_flat),
                *[pl.BlockSpec(memory_space=pl.ANY)] * 4,
                pl.BlockSpec((heads, size, width), mine),
                pl.BlockSpec((heads, width, size), mine),
            ],
            out_specs=pl.BlockSpec((rows, heads * size), lambda i, me_ref, table_ref: (0, i)),
            scratch_shapes=[
                pltpu.VMEM((keys, depth), jnp.bfloat16),
                pltpu.VMEM((rows, keys), jnp.float32),
                pltpu.VMEM((heads * rows, depth), jnp.bfloat16),
                pltpu.VMEM((heads * rows, keys), jnp.float32),
                pltpu.VMEM((heads * rows, keys), jnp.bfloat16),
                pltpu.VMEM((heads * rows, 1), jnp.float32),
                pltpu.SemaphoreType.DMA((4,)),
            ],
        ),
        out_shape=jax.ShapeDtypeStruct((rows, half // groups * size), jnp.bfloat16),
        compiler_params=pltpu.CompilerParams(vmem_limit_bytes=24 * 1024 * 1024),
        cost_estimate=pl.CostEstimate(
            flops=2 * half // groups * rows * keys * (depth + width),
            bytes_accessed=half // groups * (rows + 2 * width) * size * 2,
            transcendentals=half // groups * rows * keys,
        ),
        name="attend",
    )(me, table, *nope, *rope, *parts, wk, wv)


def project_kernel(plain, choice, prev, me_ref, *refs):
    refs = list(refs)

    def take(count):
        out, refs[:count] = refs[:count], []
        return out

    fixed = [take(2) for _ in range(plain)]
    options = [[take(2) for _ in range(choice)] for _ in range(2)]
    weights = take(len(refs) - 2 - (2 if prev else 0))
    before = take(2) if prev else []
    keep_ref, send_ref = refs
    tok = keep_ref.shape[2]
    for old, new in zip(before, refs):
        new[: old.shape[0], : old.shape[1]] = old[...]

    def emit(blocks, at, pieces):
        for j in pieces:
            total = 0.0
            for g in range(2):
                rows = jnp.concatenate([block[g][...] for block in blocks], axis=0)
                width = rows.shape[1]
                total = total + lax.dot_general(
                    rows,
                    weights[j][:, g * width : (g + 1) * width],
                    (((1,), (1,)), ((), ())),
                    preferred_element_type=jnp.float32,
                )
            for n in range(len(blocks)):
                start = 2 * tok * n
                keep_ref[j, at + n] = total[start : start + tok]
                send_ref[j, at + n] = total[start + tok : start + 2 * tok].astype(send_ref.dtype)

    pieces = range(len(weights))
    if prev:
        done, count = before[0].shape[:2]
        emit(fixed, 0, pieces[done:])
        emit(fixed[count:], count, pieces[:done])
    elif fixed:
        emit(fixed, 0, pieces)
    slab = me_ref[0] >> 2
    inner = (slab == 1) | (slab == 2)
    for n, option in enumerate(options):
        if option:

            @pl.when(inner if n == 0 else ~inner)
            def _():
                emit(option, plain, pieces)


def project(me, fixed, options, weights, tok, before=()):
    count = len(fixed) + len(options) // 2
    shape = (len(weights), count, tok, weights[0].shape[0])
    operands = [ref for block in [*fixed, *options] for ref in block] + list(weights) + list(before)
    vmem = pl.BlockSpec(memory_space=pltpu.VMEM)
    return pl.pallas_call(
        functools.partial(project_kernel, len(fixed), len(options) // 2, bool(before)),
        in_specs=[pl.BlockSpec(memory_space=pltpu.SMEM)] + [vmem] * len(operands),
        out_specs=[vmem, vmem],
        out_shape=[
            jax.ShapeDtypeStruct(shape, jnp.float32),
            jax.ShapeDtypeStruct(shape, jnp.bfloat16),
        ],
        compiler_params=pltpu.CompilerParams(vmem_limit_bytes=6 * 1024 * 1024),
        cost_estimate=pl.CostEstimate(
            flops=4 * tok * count * sum(w.size for w in weights),
            bytes_accessed=0,
            transcendentals=0,
        ),
        name="project",
    )(me, *operands)


def halve_kernel(x_ref, keep_ref, other_ref, mine_ref, send_ref):
    pieces, count, tok, _ = keep_ref.shape
    for j in range(pieces):
        for n in range(count):
            total = keep_ref[j, n] + other_ref[j ^ 1, n].astype(jnp.float32)
            low, high = total[: tok // 2], total[tok // 2 :]

            @pl.when(x_ref[0] == 0)
            def _():
                mine_ref[j, n] = low
                send_ref[j, n] = high.astype(send_ref.dtype)

            @pl.when(x_ref[0] != 0)
            def _():
                mine_ref[j, n] = high
                send_ref[j, n] = low.astype(send_ref.dtype)


def join_kernel(mine_ref, got_ref, *outs):
    for n, out in enumerate(outs):
        for j in range(mine_ref.shape[0]):
            out[j] = (mine_ref[j, n] + got_ref[j, n].astype(jnp.float32)).astype(out.dtype)


def halve(x, keep, other):
    pieces, count, tok, cols = keep.shape
    vmem = pl.BlockSpec(memory_space=pltpu.VMEM)
    shape = (pieces, count, tok // 2, cols)
    return pl.pallas_call(
        halve_kernel,
        in_specs=[pl.BlockSpec(memory_space=pltpu.SMEM), vmem, vmem],
        out_specs=[vmem, vmem],
        out_shape=[
            jax.ShapeDtypeStruct(shape, jnp.float32),
            jax.ShapeDtypeStruct(shape, jnp.bfloat16),
        ],
        compiler_params=pltpu.CompilerParams(vmem_limit_bytes=4 * 1024 * 1024),
        name="halve",
    )(x, keep, other)


def join(mine, got):
    pieces, count, tok, cols = mine.shape
    vmem = pl.BlockSpec(memory_space=pltpu.VMEM)
    return pl.pallas_call(
        join_kernel,
        in_specs=[vmem, vmem],
        out_specs=[vmem] * count,
        out_shape=[jax.ShapeDtypeStruct((pieces, tok, cols), jnp.bfloat16)] * count,
        compiler_params=pltpu.CompilerParams(vmem_limit_bytes=4 * 1024 * 1024),
        name="join",
    )(mine, got)


def finish_kernel(me_ref, res_ref, gain_ref, *refs):
    pieces = refs[:-3]
    new_ref, normed_ref, hidden_ref = refs[-3:]
    me = me_ref[0]
    cols = pieces[0].shape[2]
    wide = 4 * cols
    for k, piece in enumerate(pieces):
        at = pl.multiple_of(((me >> 2) ^ k) * wide, wide)
        for case in range(4):

            @pl.when((me & 3) == case)
            def _():
                row = jnp.concatenate([piece[j ^ case] for j in range(4)], axis=1)
                old = res_ref[:, pl.ds(at, wide)].astype(jnp.float32)
                hidden_ref[:, pl.ds(at, wide)] = old + row.astype(jnp.float32)

    hidden = hidden_ref[...]
    new_ref[...] = hidden.astype(new_ref.dtype)
    scale = lax.rsqrt(jnp.mean(hidden * hidden, axis=1, keepdims=True) + 1e-06)
    normed_ref[...] = (hidden * scale * gain_ref[...]).astype(normed_ref.dtype)


def finish(me, residual, gain, pieces):
    vmem = pl.BlockSpec(memory_space=pltpu.VMEM)
    out = jax.ShapeDtypeStruct(residual.shape, jnp.bfloat16)
    return pl.pallas_call(
        finish_kernel,
        in_specs=[pl.BlockSpec(memory_space=pltpu.SMEM)] + [vmem] * (2 + len(pieces)),
        out_specs=[vmem, vmem],
        out_shape=[out, out],
        scratch_shapes=[pltpu.VMEM(residual.shape, jnp.float32)],
        compiler_params=pltpu.CompilerParams(vmem_limit_bytes=8 * 1024 * 1024),
        name="finish",
    )(me, residual, gain, *pieces)


def per_device(
    q_nope, q_rope, latent, key_rope, absorb_key, absorb_value, w_out, residual, norm_gain, span_table
):
    f32, bf16 = jnp.float32, jnp.bfloat16
    tok, heads, size = q_nope.shape
    rope = q_rope.shape[2]
    n_seq, n_heads = lax.axis_size("seq"), lax.axis_size("heads")
    depth_z = n_seq // 4
    me = lax.axis_index("seq").astype(jnp.int32)
    core, slab = me & 1, me >> 2
    half = heads // 2

    line = depth_z == 4

    def swap(x, bit):
        return lax.ppermute(x, "seq", [(i, i ^ bit) for i in range(n_seq)])

    def move(x, pairs):
        return lax.ppermute(x, "seq", [(4 * a + r, 4 * b + r) for a, b in pairs for r in range(4)])

    kv_own = pack(latent, key_rope.T)
    zs, ys = [kv_own], [swap(kv_own, 2)]
    for k in range(1, depth_z):
        k = (k ^ (k >> 1)) if line else k
        zs.append(swap(kv_own, 4 * k))
        ys.append(swap(zs[-1], 2))
    if line:
        zs, ys = [zs[k] for k in (0, 1, 3, 2)], [ys[k] for k in (0, 1, 3, 2)]
    along, across = jnp.concatenate(zs, axis=0), jnp.concatenate(ys, axis=0)

    def split_heads(x, count):
        mine = lax.dynamic_slice_in_dim(x, core * count, count, 0)
        theirs = lax.dynamic_slice_in_dim(x, (1 - core) * count, count, 0)
        return mine, swap(theirs, 1)

    nope = split_heads(jnp.transpose(q_nope, (1, 0, 2)), half)
    rotary = split_heads(jnp.transpose(q_rope, (1, 2, 0)).reshape(heads * rope, tok), half * rope)

    wk = lax.dynamic_slice_in_dim(absorb_key, core * half, half, 0)
    wv = lax.dynamic_slice_in_dim(absorb_value, core * half, half, 0)
    head_group = lax.axis_index("heads").astype(jnp.int32).reshape(1)
    gain = norm_gain[None, :]
    along, head_group, gain, *own = lax.optimization_barrier(
        (along, head_group, gain, nope[0], rotary[0])
    )
    nope, rotary = (own[0], nope[1]), (own[1], rotary[1])
    parts = [along, across, swap(along, 1), swap(across, 1)]

    w_t = w_out.T
    cols = w_t.shape[0]
    span = half * size
    w_mine = lax.dynamic_slice_in_dim(w_t, core * span, span, 1)
    w_theirs = lax.dynamic_slice_in_dim(w_t, (1 - core) * span, span, 1)
    w_core = swap(w_theirs, 1)
    weights = [w_mine, w_core, swap(w_mine, 2), swap(w_core, 2)]

    groups = 2
    step_heads = max(
        h for h in (4, 2) if half // groups % h == 0 and h * tok * 8 * tok * depth_z <= 3 << 19
    )
    blocks = []
    for g in range(groups):
        mixed = attend(
            me.reshape(1),
            span_table,
            nope,
            rotary,
            parts,
            wk,
            wv,
            g,
            groups,
            step_heads,
        )
        if line:
            near, opposite = swap(mixed, 4), swap(mixed, 12)
            far = move(near, [(1, 2), (2, 1)])
            out = move(opposite, [(1, 0), (2, 3)])
            blocks.append([mixed, near, opposite, far, out])
        else:
            blocks.append([mixed] + [swap(mixed, 4 * k) for k in range(1, depth_z)])

    def reduce(keep, send):
        count = keep.shape[1]
        other = swap(send, 1)
        if n_heads == 2:
            mine, send = halve(head_group, keep, other)
            got = lax.ppermute(send, "heads", [(0, 1), (1, 0)])
            return list(join(mine, got))
        total = keep + jnp.stack([other[j ^ 1] for j in range(4)]).astype(f32)
        total = lax.psum_scatter(total.astype(bf16), "heads", scatter_dimension=2, tiled=True)
        return [total[:, n] for n in range(count)]

    if line:
        mixed, near, opposite, far, out = zip(*blocks)
        me1 = me.reshape(1)
        first = project(me1, [mixed, near], [], weights[:2], tok)
        early = project(me1, [mixed, near, opposite], [], weights, tok, first)
        late = project(me1, [], [far, out], weights, tok)
        mine = reduce(*early) + reduce(*late)
        mine[2], mine[3] = mine[3], mine[2]
    else:
        rows = jnp.stack([jnp.concatenate(parts, axis=1) for parts in zip(*blocks)])
        total = jnp.einsum("zti,joi->jzto", rows, jnp.stack(weights), preferred_element_type=f32)
        mine = reduce(total[:, :, :tok], total[:, :, tok:].astype(bf16))
    pieces = [mine[0]] + [swap(mine[k], 4 * k) for k in range(1, depth_z)]
    if 4 * cols % 128 == 0:
        return tuple(finish(me.reshape(1), residual, gain, pieces))
    places = slab ^ jnp.arange(depth_z, dtype=jnp.int32)
    order = jnp.arange(depth_z, dtype=jnp.int32)
    order = jnp.sum(jnp.where(places[None, :] == order[:, None], order[None, :], 0), axis=1)
    columns = jnp.take(jnp.stack(pieces), order, axis=0)
    columns = jnp.take(columns, jnp.arange(4, dtype=jnp.int32) ^ (me & 3), axis=1)
    hidden = residual.astype(f32) + jnp.moveaxis(columns, 2, 0).reshape(residual.shape).astype(f32)
    scale = lax.rsqrt(jnp.mean(hidden * hidden, axis=1, keepdims=True) + 1e-06)
    return (hidden.astype(bf16), (hidden * scale * gain).astype(bf16))


def solution(mesh):
    in_specs = (
        P("seq", "heads", None),
        P("seq", "heads", None),
        P("seq", None),
        P("seq", None),
        P("heads", None, None),
        P("heads", None, None),
        P("heads", "seq"),
        P(("seq", "heads"), None),
        P(),
        P(),
    )
    out_specs = (P(("seq", "heads"), None), P(("seq", "heads"), None))

    return jax.shard_map(
        per_device, mesh=mesh, in_specs=in_specs, out_specs=out_specs, check_vma=False
    )
```

```python
import functools

import jax
import jax.numpy as jnp
from jax import lax
from jax.experimental import pallas as pl
from jax.experimental.pallas import tpu as pltpu
from jax.sharding import PartitionSpec as P

score_scale = 192.0 ** (-0.5)
LOG2E = 1.4426950408889634


def pack_kernel(lat_ref, rope_ref, out_ref, held_ref, sem):
    width = lat_ref.shape[1]
    copies = [
        pltpu.make_async_copy(lat_ref, out_ref.at[:, pl.ds(0, width)], sem.at[0]),
        pltpu.make_async_copy(rope_ref, held_ref, sem.at[1]),
    ]
    for copy in copies:
        copy.start()
    copies[1].wait()
    rope = held_ref[...].astype(jnp.float32).T
    both = jnp.concatenate([rope, rope], axis=1)
    out_ref[:, width:] = both.astype(out_ref.dtype)
    copies[0].wait()


def pack(latent, rope_t):
    return pl.pallas_call(
        pack_kernel,
        out_shape=jax.ShapeDtypeStruct(
            (latent.shape[0], latent.shape[1] + 2 * rope_t.shape[0]), latent.dtype
        ),
        in_specs=[pl.BlockSpec(memory_space=pltpu.HBM)] * 2,
        out_specs=pl.BlockSpec(memory_space=pltpu.VMEM),
        scratch_shapes=[pltpu.VMEM(rope_t.shape, rope_t.dtype), pltpu.SemaphoreType.DMA((2,))],
        compiler_params=pltpu.CompilerParams(vmem_limit_bytes=8 * 1024 * 1024),
        name="pack",
    )(latent, rope_t)


def attend_kernel(
    me_ref,
    table_ref,
    nope0_ref,
    nope1_ref,
    rope0_ref,
    rope1_ref,
    *refs,
):
    parts = refs[:4]
    wk_ref, wv_ref, out_ref, kv_ref, bias_ref, q_ref, s_ref, p_ref, total_ref, sem = refs[4:]
    heads, tok, _ = nope0_ref.shape
    rows, keys = bias_ref.shape
    width = wk_ref.shape[2]
    rope = rope0_ref.shape[0] // heads
    span_len = keys // table_ref.shape[0]
    per = tok // span_len

    length = keys // 4
    copies = [
        pltpu.make_async_copy(part, kv_ref.at[pl.ds(n * length, length)], sem.at[n])
        for n, part in enumerate(parts)
    ]

    @pl.when(pl.program_id(0) == 0)
    def _():
        for copy in copies:
            copy.start()
        me = me_ref[0]
        slabs = length // tok
        lane = lax.broadcasted_iota(jnp.int32, (1, keys), 1)
        kpos = jnp.zeros((1, keys), jnp.int32)
        for n in range(keys // span_len):
            block, inside = n // per, n % per
            part, k = block // slabs, block % slabs
            slab = (me >> 2) ^ k
            source = slab * 4 + ((me & 3) ^ ((part & 1) * 2 + (part >> 1)))
            first = table_ref[source * per + inside] * span_len - n * span_len
            kpos = jnp.where(lane >= n * span_len, first + lane, kpos)
        sub = lax.broadcasted_iota(jnp.int32, (rows, 1), 0)
        qpos = jnp.zeros((rows, 1), jnp.int32)
        for n in range(rows // span_len):
            source = me ^ (n // per)
            first = table_ref[source * per + n % per] * span_len - n * span_len
            qpos = jnp.where(sub >= n * span_len, first + sub, qpos)
        bias_ref[...] = jnp.where(kpos <= qpos, jnp.float32(0.0), jnp.float32(-1e30))

    f32, bf16 = jnp.float32, jnp.bfloat16
    for h in range(heads):
        nope = jnp.concatenate([nope0_ref[h].astype(f32), nope1_ref[h].astype(f32)], axis=0)
        q_lat = jnp.dot(nope.astype(bf16), wk_ref[h], preferred_element_type=f32)
        q_ref[h * rows : (h + 1) * rows, :width] = q_lat.astype(bf16)
    lane = lax.broadcasted_iota(jnp.int32, (rows, 2 * rope), 1)
    for h in range(0, heads, 2):
        pick = slice(h * rope, (h + 2) * rope)
        pair = jnp.concatenate(
            [rope0_ref[pick, :].astype(f32).T, rope1_ref[pick, :].astype(f32).T], axis=0
        )
        q_ref[h * rows : (h + 1) * rows, width:] = jnp.where(lane < rope, pair, 0.0).astype(bf16)
        q_ref[(h + 1) * rows : (h + 2) * rows, width:] = jnp.where(lane < rope, 0.0, pair).astype(
            bf16
        )

    @pl.when(pl.program_id(0) == 0)
    def _():
        for copy in copies:
            copy.wait()

    units, step = 2, 16
    count = heads * rows // units

    def scores(u):
        s_ref[pl.ds(u * count, count), :] = lax.dot_general(
            q_ref[pl.ds(u * count, count), :],
            kv_ref[...],
            (((1,), (1,)), ((), ())),
            preferred_element_type=f32,
        )

    def weights(u):
        for r in range(u * count, (u + 1) * count, step):
            block = s_ref[r : r + step, :] * (score_scale * LOG2E)
            block = block + bias_ref[r % rows : r % rows + step, :]
            weight = jnp.exp2(block - jnp.max(block, axis=1, keepdims=True))
            total_ref[r : r + step, :] = 1.0 / jnp.sum(weight, axis=1, keepdims=True)
            p_ref[r : r + step, :] = weight.astype(bf16)

    def outputs(u):
        context = jnp.dot(
            p_ref[pl.ds(u * count, count), :], kv_ref[:, :width], preferred_element_type=f32
        )
        context = (context * total_ref[pl.ds(u * count, count), :]).astype(bf16)
        for n in range(count // rows):
            h = u * (count // rows) + n
            part = jnp.dot(
                context[n * rows : (n + 1) * rows], wv_ref[h], preferred_element_type=f32
            )
            out_ref[:, h * part.shape[1] : (h + 1) * part.shape[1]] = part.astype(out_ref.dtype)

    for u in range(units + 2):
        if u < units:
            scores(u)
        if 1 <= u <= units:
            weights(u - 1)
        if u >= 2:
            outputs(u - 2)


def attend(me, table, nope, rope, parts, wk, wv, group, groups, heads):
    half, tok, size = nope[0].shape
    steps = half // groups // heads
    rows = 2 * tok
    keys, depth = 4 * parts[0].shape[0], parts[0].shape[1]
    width = wk.shape[2]
    rope_rows = rope[0].shape[0] // half * heads
    first = group * steps

    def mine(i, me_ref, table_ref):
        return (first + i, 0, 0)

    def mine_flat(i, me_ref, table_ref):
        return (first + i, 0)

    return pl.pallas_call(
        attend_kernel,
        grid_spec=pltpu.PrefetchScalarGridSpec(
            num_scalar_prefetch=2,
            grid=(steps,),
            in_specs=[
                pl.BlockSpec((heads, tok, size), mine),
                pl.BlockSpec((heads, tok, size), mine),
                pl.BlockSpec((rope_rows, tok), mine_flat),
                pl.BlockSpec((rope_rows, tok), mine_flat),
                *[pl.BlockSpec(memory_space=pl.ANY)] * 4,
                pl.BlockSpec((heads, size, width), mine),
                pl.BlockSpec((heads, width, size), mine),
            ],
            out_specs=pl.BlockSpec((rows, heads * size), lambda i, me_ref, table_ref: (0, i)),
            scratch_shapes=[
                pltpu.VMEM((keys, depth), jnp.bfloat16),
                pltpu.VMEM((rows, keys), jnp.float32),
                pltpu.VMEM((heads * rows, depth), jnp.bfloat16),
                pltpu.VMEM((heads * rows, keys), jnp.float32),
                pltpu.VMEM((heads * rows, keys), jnp.bfloat16),
                pltpu.VMEM((heads * rows, 1), jnp.float32),
                pltpu.SemaphoreType.DMA((4,)),
            ],
        ),
        out_shape=jax.ShapeDtypeStruct((rows, half // groups * size), jnp.bfloat16),
        compiler_params=pltpu.CompilerParams(vmem_limit_bytes=24 * 1024 * 1024),
        cost_estimate=pl.CostEstimate(
            flops=2 * half // groups * rows * keys * (depth + width),
            bytes_accessed=half // groups * (rows + 2 * width) * size * 2,
            transcendentals=half // groups * rows * keys,
        ),
        name="attend",
    )(me, table, *nope, *rope, *parts, wk, wv)


def project_kernel(plain, choice, prev, me_ref, *refs):
    refs = list(refs)

    def take(count):
        out, refs[:count] = refs[:count], []
        return out

    fixed = [take(2) for _ in range(plain)]
    options = [[take(2) for _ in range(choice)] for _ in range(2)]
    weights = take(len(refs) - 2 - (2 if prev else 0))
    before = take(2) if prev else []
    keep_ref, send_ref = refs
    tok = keep_ref.shape[2]
    for old, new in zip(before, refs):
        new[: old.shape[0], : old.shape[1]] = old[...]

    def emit(blocks, at, pieces):
        for j in pieces:
            total = 0.0
            for g in range(2):
                rows = jnp.concatenate([block[g][...] for block in blocks], axis=0)
                width = rows.shape[1]
                total = total + lax.dot_general(
                    rows,
                    weights[j][:, g * width : (g + 1) * width],
                    (((1,), (1,)), ((), ())),
                    preferred_element_type=jnp.float32,
                )
            for n in range(len(blocks)):
                start = 2 * tok * n
                keep_ref[j, at + n] = total[start : start + tok]
                send_ref[j, at + n] = total[start + tok : start + 2 * tok].astype(send_ref.dtype)

    pieces = range(len(weights))
    if prev:
        done, count = before[0].shape[:2]
        emit(fixed, 0, pieces[done:])
        if fixed[count:]:
            emit(fixed[count:], count, pieces[:done])
    elif fixed:
        emit(fixed, 0, pieces)
    slab = me_ref[0] >> 2
    inner = (slab == 1) | (slab == 2)
    for n, option in enumerate(options):
        if option:

            @pl.when(inner if n == 0 else ~inner)
            def _():
                emit(option, plain, pieces)


def project(me, fixed, options, weights, tok, before=()):
    count = len(fixed) + len(options) // 2
    shape = (len(weights), count, tok, weights[0].shape[0])
    operands = [ref for block in [*fixed, *options] for ref in block] + list(weights) + list(before)
    vmem = pl.BlockSpec(memory_space=pltpu.VMEM)
    return pl.pallas_call(
        functools.partial(project_kernel, len(fixed), len(options) // 2, bool(before)),
        in_specs=[pl.BlockSpec(memory_space=pltpu.SMEM)] + [vmem] * len(operands),
        out_specs=[vmem, vmem],
        out_shape=[
            jax.ShapeDtypeStruct(shape, jnp.float32),
            jax.ShapeDtypeStruct(shape, jnp.bfloat16),
        ],
        compiler_params=pltpu.CompilerParams(vmem_limit_bytes=6 * 1024 * 1024),
        cost_estimate=pl.CostEstimate(
            flops=4 * tok * count * sum(w.size for w in weights),
            bytes_accessed=0,
            transcendentals=0,
        ),
        name="project",
    )(me, *operands)


def halve_kernel(x_ref, keep_ref, other_ref, mine_ref, send_ref):
    pieces, count, tok, _ = keep_ref.shape
    for j in range(pieces):
        for n in range(count):
            total = keep_ref[j, n] + other_ref[j ^ 1, n].astype(jnp.float32)
            low, high = total[: tok // 2], total[tok // 2 :]

            @pl.when(x_ref[0] == 0)
            def _():
                mine_ref[j, n] = low
                send_ref[j, n] = high.astype(send_ref.dtype)

            @pl.when(x_ref[0] != 0)
            def _():
                mine_ref[j, n] = high
                send_ref[j, n] = low.astype(send_ref.dtype)


def join_kernel(mine_ref, got_ref, *outs):
    for n, out in enumerate(outs):
        for j in range(mine_ref.shape[0]):
            out[j] = (mine_ref[j, n] + got_ref[j, n].astype(jnp.float32)).astype(out.dtype)


def halve(x, keep, other):
    pieces, count, tok, cols = keep.shape
    vmem = pl.BlockSpec(memory_space=pltpu.VMEM)
    shape = (pieces, count, tok // 2, cols)
    return pl.pallas_call(
        halve_kernel,
        in_specs=[pl.BlockSpec(memory_space=pltpu.SMEM), vmem, vmem],
        out_specs=[vmem, vmem],
        out_shape=[
            jax.ShapeDtypeStruct(shape, jnp.float32),
            jax.ShapeDtypeStruct(shape, jnp.bfloat16),
        ],
        compiler_params=pltpu.CompilerParams(vmem_limit_bytes=4 * 1024 * 1024),
        name="halve",
    )(x, keep, other)


def join(mine, got):
    pieces, count, tok, cols = mine.shape
    vmem = pl.BlockSpec(memory_space=pltpu.VMEM)
    return pl.pallas_call(
        join_kernel,
        in_specs=[vmem, vmem],
        out_specs=[vmem] * count,
        out_shape=[jax.ShapeDtypeStruct((pieces, tok, cols), jnp.bfloat16)] * count,
        compiler_params=pltpu.CompilerParams(vmem_limit_bytes=4 * 1024 * 1024),
        name="join",
    )(mine, got)


def finish_kernel(me_ref, res_ref, gain_ref, *refs):
    pieces = refs[:-3]
    new_ref, normed_ref, hidden_ref = refs[-3:]
    me = me_ref[0]
    cols = pieces[0].shape[2]
    wide = 4 * cols
    for k, piece in enumerate(pieces):
        at = pl.multiple_of(((me >> 2) ^ k) * wide, wide)
        for case in range(4):

            @pl.when((me & 3) == case)
            def _():
                row = jnp.concatenate([piece[j ^ case] for j in range(4)], axis=1)
                old = res_ref[:, pl.ds(at, wide)].astype(jnp.float32)
                hidden_ref[:, pl.ds(at, wide)] = old + row.astype(jnp.float32)

    hidden = hidden_ref[...]
    new_ref[...] = hidden.astype(new_ref.dtype)
    scale = lax.rsqrt(jnp.mean(hidden * hidden, axis=1, keepdims=True) + 1e-06)
    normed_ref[...] = (hidden * scale * gain_ref[...]).astype(normed_ref.dtype)


def finish(me, residual, gain, pieces):
    vmem = pl.BlockSpec(memory_space=pltpu.VMEM)
    out = jax.ShapeDtypeStruct(residual.shape, jnp.bfloat16)
    return pl.pallas_call(
        finish_kernel,
        in_specs=[pl.BlockSpec(memory_space=pltpu.SMEM)] + [vmem] * (2 + len(pieces)),
        out_specs=[vmem, vmem],
        out_shape=[out, out],
        scratch_shapes=[pltpu.VMEM(residual.shape, jnp.float32)],
        compiler_params=pltpu.CompilerParams(vmem_limit_bytes=8 * 1024 * 1024),
        name="finish",
    )(me, residual, gain, *pieces)


def per_device(
    q_nope, q_rope, latent, key_rope, absorb_key, absorb_value, w_out, residual, norm_gain, span_table
):
    f32, bf16 = jnp.float32, jnp.bfloat16
    tok, heads, size = q_nope.shape
    rope = q_rope.shape[2]
    n_seq, n_heads = lax.axis_size("seq"), lax.axis_size("heads")
    depth_z = n_seq // 4
    me = lax.axis_index("seq").astype(jnp.int32)
    core, slab = me & 1, me >> 2
    half = heads // 2

    line = depth_z == 4

    def swap(x, bit):
        return lax.ppermute(x, "seq", [(i, i ^ bit) for i in range(n_seq)])

    def move(x, pairs):
        return lax.ppermute(x, "seq", [(4 * a + r, 4 * b + r) for a, b in pairs for r in range(4)])

    kv_own = pack(latent, key_rope.T)
    zs, ys = [kv_own], [swap(kv_own, 2)]
    for k in range(1, depth_z):
        k = (k ^ (k >> 1)) if line else k
        zs.append(swap(kv_own, 4 * k))
        ys.append(swap(zs[-1], 2))
    if line:
        zs, ys = [zs[k] for k in (0, 1, 3, 2)], [ys[k] for k in (0, 1, 3, 2)]
    along, across = jnp.concatenate(zs, axis=0), jnp.concatenate(ys, axis=0)

    def split_heads(x, count):
        mine = lax.dynamic_slice_in_dim(x, core * count, count, 0)
        theirs = lax.dynamic_slice_in_dim(x, (1 - core) * count, count, 0)
        return mine, swap(theirs, 1)

    nope = split_heads(jnp.transpose(q_nope, (1, 0, 2)), half)
    rotary = split_heads(jnp.transpose(q_rope, (1, 2, 0)).reshape(heads * rope, tok), half * rope)

    wk = lax.dynamic_slice_in_dim(absorb_key, core * half, half, 0)
    wv = lax.dynamic_slice_in_dim(absorb_value, core * half, half, 0)
    head_group = lax.axis_index("heads").astype(jnp.int32).reshape(1)
    gain = norm_gain[None, :]
    along, head_group, gain, *own = lax.optimization_barrier(
        (along, head_group, gain, nope[0], rotary[0])
    )
    nope, rotary = (own[0], nope[1]), (own[1], rotary[1])
    parts = [along, across, swap(along, 1), swap(across, 1)]

    w_t = w_out.T
    cols = w_t.shape[0]
    span = half * size
    w_mine = lax.dynamic_slice_in_dim(w_t, core * span, span, 1)
    w_theirs = lax.dynamic_slice_in_dim(w_t, (1 - core) * span, span, 1)
    w_core = swap(w_theirs, 1)
    weights = [w_mine, w_core, swap(w_mine, 2), swap(w_core, 2)]

    groups = 2
    step_heads = max(
        h for h in (4, 2) if half // groups % h == 0 and h * tok * 8 * tok * depth_z <= 3 << 19
    )
    blocks = []
    for g in range(groups):
        mixed = attend(
            me.reshape(1),
            span_table,
            nope,
            rotary,
            parts,
            wk,
            wv,
            g,
            groups,
            step_heads,
        )
        if line:
            near, opposite = swap(mixed, 4), swap(mixed, 12)
            far = move(near, [(1, 2), (2, 1)])
            out = move(opposite, [(1, 0), (2, 3)])
            blocks.append([mixed, near, opposite, far, out])
        else:
            blocks.append([mixed] + [swap(mixed, 4 * k) for k in range(1, depth_z)])

    def reduce(keep, send):
        count = keep.shape[1]
        other = swap(send, 1)
        if n_heads == 2:
            mine, send = halve(head_group, keep, other)
            got = lax.ppermute(send, "heads", [(0, 1), (1, 0)])
            return list(join(mine, got))
        total = keep + jnp.stack([other[j ^ 1] for j in range(4)]).astype(f32)
        total = lax.psum_scatter(total.astype(bf16), "heads", scatter_dimension=2, tiled=True)
        return [total[:, n] for n in range(count)]

    if line:
        mixed, near, opposite, far, out = zip(*blocks)
        me1 = me.reshape(1)
        first = project(me1, [mixed, near], [], weights[:2], tok)
        early = project(me1, [mixed, near], [], weights, tok, first)
        middle = project(me1, [opposite], [], weights, tok)
        late = project(me1, [], [far, out], weights, tok)
        mine = reduce(*early) + reduce(*late) + reduce(*middle)
    else:
        rows = jnp.stack([jnp.concatenate(parts, axis=1) for parts in zip(*blocks)])
        total = jnp.einsum("zti,joi->jzto", rows, jnp.stack(weights), preferred_element_type=f32)
        mine = reduce(total[:, :, :tok], total[:, :, tok:].astype(bf16))
    pieces = [mine[0]] + [swap(mine[k], 4 * k) for k in range(1, depth_z)]
    if 4 * cols % 128 == 0:
        return tuple(finish(me.reshape(1), residual, gain, pieces))
    places = slab ^ jnp.arange(depth_z, dtype=jnp.int32)
    order = jnp.arange(depth_z, dtype=jnp.int32)
    order = jnp.sum(jnp.where(places[None, :] == order[:, None], order[None, :], 0), axis=1)
    columns = jnp.take(jnp.stack(pieces), order, axis=0)
    columns = jnp.take(columns, jnp.arange(4, dtype=jnp.int32) ^ (me & 3), axis=1)
    hidden = residual.astype(f32) + jnp.moveaxis(columns, 2, 0).reshape(residual.shape).astype(f32)
    scale = lax.rsqrt(jnp.mean(hidden * hidden, axis=1, keepdims=True) + 1e-06)
    return (hidden.astype(bf16), (hidden * scale * gain).astype(bf16))


def solution(mesh):
    in_specs = (
        P("seq", "heads", None),
        P("seq", "heads", None),
        P("seq", None),
        P("seq", None),
        P("heads", None, None),
        P("heads", None, None),
        P("heads", "seq"),
        P(("seq", "heads"), None),
        P(),
        P(),
    )
    out_specs = (P(("seq", "heads"), None), P(("seq", "heads"), None))

    return jax.shard_map(
        per_device, mesh=mesh, in_specs=in_specs, out_specs=out_specs, check_vma=False
    )
```

```python
import functools

import jax
import jax.numpy as jnp
from jax import lax
from jax.experimental import pallas as pl
from jax.experimental.pallas import tpu as pltpu
from jax.sharding import PartitionSpec as P

score_scale = 192.0 ** (-0.5)
LOG2E = 1.4426950408889634


def pack_kernel(lat_ref, rope_ref, out_ref, held_ref, sem):
    width = lat_ref.shape[1]
    copies = [
        pltpu.make_async_copy(lat_ref, out_ref.at[:, pl.ds(0, width)], sem.at[0]),
        pltpu.make_async_copy(rope_ref, held_ref, sem.at[1]),
    ]
    for copy in copies:
        copy.start()
    copies[1].wait()
    rope = held_ref[...].astype(jnp.float32).T
    both = jnp.concatenate([rope, rope], axis=1)
    out_ref[:, width:] = both.astype(out_ref.dtype)
    copies[0].wait()


def pack(latent, rope_t):
    return pl.pallas_call(
        pack_kernel,
        out_shape=jax.ShapeDtypeStruct(
            (latent.shape[0], latent.shape[1] + 2 * rope_t.shape[0]), latent.dtype
        ),
        in_specs=[pl.BlockSpec(memory_space=pltpu.HBM)] * 2,
        out_specs=pl.BlockSpec(memory_space=pltpu.VMEM),
        scratch_shapes=[pltpu.VMEM(rope_t.shape, rope_t.dtype), pltpu.SemaphoreType.DMA((2,))],
        compiler_params=pltpu.CompilerParams(vmem_limit_bytes=8 * 1024 * 1024),
        name="pack",
    )(latent, rope_t)


def attend_kernel(
    first,
    steps,
    heads,
    me_ref,
    table_ref,
    nope0_ref,
    nope1_ref,
    rope0_ref,
    rope1_ref,
    *refs,
):
    parts = refs[:4]
    wk_ref, wv_ref, out_ref, kv_ref, bias_ref, q_ref, s_ref, p_ref, total_ref, sem = refs[4:]
    tok = nope0_ref.shape[1]
    rows, keys = bias_ref.shape
    width = wk_ref.shape[2]
    rope = rope0_ref.shape[0] // nope0_ref.shape[0]
    span_len = keys // table_ref.shape[0]
    per = tok // span_len

    length = keys // 4
    copies = [
        pltpu.make_async_copy(part, kv_ref.at[pl.ds(n * length, length)], sem.at[n])
        for n, part in enumerate(parts)
    ]

    def prepare():
        for copy in copies:
            copy.start()
        me = me_ref[0]
        slabs = length // tok
        lane = lax.broadcasted_iota(jnp.int32, (1, keys), 1)
        kpos = jnp.zeros((1, keys), jnp.int32)
        for n in range(keys // span_len):
            block, inside = n // per, n % per
            part, k = block // slabs, block % slabs
            slab = (me >> 2) ^ k
            source = slab * 4 + ((me & 3) ^ ((part & 1) * 2 + (part >> 1)))
            first = table_ref[source * per + inside] * span_len - n * span_len
            kpos = jnp.where(lane >= n * span_len, first + lane, kpos)
        sub = lax.broadcasted_iota(jnp.int32, (rows, 1), 0)
        qpos = jnp.zeros((rows, 1), jnp.int32)
        for n in range(rows // span_len):
            source = me ^ (n // per)
            first = table_ref[source * per + n % per] * span_len - n * span_len
            qpos = jnp.where(sub >= n * span_len, first + sub, qpos)
        bias_ref[...] = jnp.where(kpos <= qpos, jnp.float32(0.0), jnp.float32(-1e30))

    f32, bf16 = jnp.float32, jnp.bfloat16

    def queries(base):
        for h in range(heads):
            g = base + h
            nope = jnp.concatenate([nope0_ref[g].astype(f32), nope1_ref[g].astype(f32)], axis=0)
            q_lat = jnp.dot(nope.astype(bf16), wk_ref[g], preferred_element_type=f32)
            q_ref[h * rows : (h + 1) * rows, :width] = q_lat.astype(bf16)
        lane = lax.broadcasted_iota(jnp.int32, (rows, 2 * rope), 1)
        for h in range(0, heads, 2):
            pick = slice((base + h) * rope, (base + h + 2) * rope)
            pair = jnp.concatenate(
                [rope0_ref[pick, :].astype(f32).T, rope1_ref[pick, :].astype(f32).T], axis=0
            )
            q_ref[h * rows : (h + 1) * rows, width:] = jnp.where(lane < rope, pair, 0.0).astype(bf16)
            q_ref[(h + 1) * rows : (h + 2) * rows, width:] = jnp.where(lane < rope, 0.0, pair).astype(
                bf16
            )

    def attention(base, at):
        units, step = 2, 16
        count = heads * rows // units

        def scores(u):
            s_ref[pl.ds(u * count, count), :] = lax.dot_general(
                q_ref[pl.ds(u * count, count), :],
                kv_ref[...],
                (((1,), (1,)), ((), ())),
                preferred_element_type=f32,
            )

        def weights(u):
            for r in range(u * count, (u + 1) * count, step):
                block = s_ref[r : r + step, :] * (score_scale * LOG2E)
                block = block + bias_ref[r % rows : r % rows + step, :]
                weight = jnp.exp2(block - jnp.max(block, axis=1, keepdims=True))
                total_ref[r : r + step, :] = 1.0 / jnp.sum(weight, axis=1, keepdims=True)
                p_ref[r : r + step, :] = weight.astype(bf16)

        def outputs(u):
            context = jnp.dot(
                p_ref[pl.ds(u * count, count), :], kv_ref[:, :width], preferred_element_type=f32
            )
            context = (context * total_ref[pl.ds(u * count, count), :]).astype(bf16)
            for n in range(count // rows):
                h = u * (count // rows) + n
                part = jnp.dot(
                    context[n * rows : (n + 1) * rows], wv_ref[base + h], preferred_element_type=f32
                )
                c = (at + h) * part.shape[1]
                out_ref[:, c : c + part.shape[1]] = part.astype(out_ref.dtype)

        for u in range(units + 2):
            if u < units:
                scores(u)
            if 1 <= u <= units:
                weights(u - 1)
            if u >= 2:
                outputs(u - 2)

    prepare()
    for n in range(steps):
        base = first + n * heads
        queries(base)
        if n == 0:
            for copy in copies:
                copy.wait()
        attention(base, n * heads)


def attend(me, table, nope, rope, parts, wk, wv, group, groups, heads):
    half, tok, size = nope[0].shape
    steps = half // groups // heads
    rows = 2 * tok
    keys, depth = 4 * parts[0].shape[0], parts[0].shape[1]
    width = wk.shape[2]
    smem, vmem = pl.BlockSpec(memory_space=pltpu.SMEM), pl.BlockSpec(memory_space=pltpu.VMEM)
    return pl.pallas_call(
        functools.partial(attend_kernel, group * steps * heads, steps, heads),
        in_specs=[smem] * 2 + [vmem] * 10,
        out_specs=vmem,
        scratch_shapes=[
            pltpu.VMEM((keys, depth), jnp.bfloat16),
            pltpu.VMEM((rows, keys), jnp.float32),
            pltpu.VMEM((heads * rows, depth), jnp.bfloat16),
            pltpu.VMEM((heads * rows, keys), jnp.float32),
            pltpu.VMEM((heads * rows, keys), jnp.bfloat16),
            pltpu.VMEM((heads * rows, 1), jnp.float32),
            pltpu.SemaphoreType.DMA((4,)),
        ],
        out_shape=jax.ShapeDtypeStruct((rows, half // groups * size), jnp.bfloat16),
        compiler_params=pltpu.CompilerParams(vmem_limit_bytes=24 * 1024 * 1024),
        cost_estimate=pl.CostEstimate(
            flops=2 * half // groups * rows * keys * (depth + width),
            bytes_accessed=half // groups * (rows + 2 * width) * size * 2,
            transcendentals=half // groups * rows * keys,
        ),
        name="attend",
    )(me, table, *nope, *rope, *parts, wk, wv)


def project_kernel(plain, choice, prev, me_ref, *refs):
    refs = list(refs)

    def take(count):
        out, refs[:count] = refs[:count], []
        return out

    fixed = [take(2) for _ in range(plain)]
    options = [[take(2) for _ in range(choice)] for _ in range(2)]
    weights = take(len(refs) - 2 - (2 if prev else 0))
    before = take(2) if prev else []
    keep_ref, send_ref = refs
    tok = keep_ref.shape[2]
    for old, new in zip(before, refs):
        new[: old.shape[0], : old.shape[1]] = old[...]

    def emit(blocks, at, pieces):
        for j in pieces:
            total = 0.0
            for g in range(2):
                rows = jnp.concatenate([block[g][...] for block in blocks], axis=0)
                width = rows.shape[1]
                total = total + lax.dot_general(
                    rows,
                    weights[j][:, g * width : (g + 1) * width],
                    (((1,), (1,)), ((), ())),
                    preferred_element_type=jnp.float32,
                )
            for n in range(len(blocks)):
                start = 2 * tok * n
                keep_ref[j, at + n] = total[start : start + tok]
                send_ref[j, at + n] = total[start + tok : start + 2 * tok].astype(send_ref.dtype)

    pieces = range(len(weights))
    if prev:
        done, count = before[0].shape[:2]
        emit(fixed, 0, pieces[done:])
        if fixed[count:]:
            emit(fixed[count:], count, pieces[:done])
    elif fixed:
        emit(fixed, 0, pieces)
    slab = me_ref[0] >> 2
    inner = (slab == 1) | (slab == 2)
    for n, option in enumerate(options):
        if option:

            @pl.when(inner if n == 0 else ~inner)
            def _():
                emit(option, plain, pieces)


def project(me, fixed, options, weights, tok, before=()):
    count = len(fixed) + len(options) // 2
    shape = (len(weights), count, tok, weights[0].shape[0])
    operands = [ref for block in [*fixed, *options] for ref in block] + list(weights) + list(before)
    vmem = pl.BlockSpec(memory_space=pltpu.VMEM)
    return pl.pallas_call(
        functools.partial(project_kernel, len(fixed), len(options) // 2, bool(before)),
        in_specs=[pl.BlockSpec(memory_space=pltpu.SMEM)] + [vmem] * len(operands),
        out_specs=[vmem, vmem],
        out_shape=[
            jax.ShapeDtypeStruct(shape, jnp.float32),
            jax.ShapeDtypeStruct(shape, jnp.bfloat16),
        ],
        compiler_params=pltpu.CompilerParams(vmem_limit_bytes=6 * 1024 * 1024),
        cost_estimate=pl.CostEstimate(
            flops=4 * tok * count * sum(w.size for w in weights),
            bytes_accessed=0,
            transcendentals=0,
        ),
        name="project",
    )(me, *operands)


def halve_kernel(x_ref, keep_ref, other_ref, mine_ref, send_ref):
    pieces, count, tok, _ = keep_ref.shape
    for j in range(pieces):
        for n in range(count):
            total = keep_ref[j, n] + other_ref[j ^ 1, n].astype(jnp.float32)
            low, high = total[: tok // 2], total[tok // 2 :]

            @pl.when(x_ref[0] == 0)
            def _():
                mine_ref[j, n] = low
                send_ref[j, n] = high.astype(send_ref.dtype)

            @pl.when(x_ref[0] != 0)
            def _():
                mine_ref[j, n] = high
                send_ref[j, n] = low.astype(send_ref.dtype)


def join_kernel(mine_ref, got_ref, *outs):
    for n, out in enumerate(outs):
        for j in range(mine_ref.shape[0]):
            out[j] = (mine_ref[j, n] + got_ref[j, n].astype(jnp.float32)).astype(out.dtype)


def halve(x, keep, other):
    pieces, count, tok, cols = keep.shape
    vmem = pl.BlockSpec(memory_space=pltpu.VMEM)
    shape = (pieces, count, tok // 2, cols)
    return pl.pallas_call(
        halve_kernel,
        in_specs=[pl.BlockSpec(memory_space=pltpu.SMEM), vmem, vmem],
        out_specs=[vmem, vmem],
        out_shape=[
            jax.ShapeDtypeStruct(shape, jnp.float32),
            jax.ShapeDtypeStruct(shape, jnp.bfloat16),
        ],
        compiler_params=pltpu.CompilerParams(vmem_limit_bytes=4 * 1024 * 1024),
        name="halve",
    )(x, keep, other)


def join(mine, got):
    pieces, count, tok, cols = mine.shape
    vmem = pl.BlockSpec(memory_space=pltpu.VMEM)
    return pl.pallas_call(
        join_kernel,
        in_specs=[vmem, vmem],
        out_specs=[vmem] * count,
        out_shape=[jax.ShapeDtypeStruct((pieces, tok, cols), jnp.bfloat16)] * count,
        compiler_params=pltpu.CompilerParams(vmem_limit_bytes=4 * 1024 * 1024),
        name="join",
    )(mine, got)


def finish_kernel(me_ref, res_ref, gain_ref, *refs):
    pieces = refs[:-3]
    new_ref, normed_ref, hidden_ref = refs[-3:]
    me = me_ref[0]
    cols = pieces[0].shape[2]
    wide = 4 * cols
    for k, piece in enumerate(pieces):
        at = pl.multiple_of(((me >> 2) ^ k) * wide, wide)
        for case in range(4):

            @pl.when((me & 3) == case)
            def _():
                row = jnp.concatenate([piece[j ^ case] for j in range(4)], axis=1)
                old = res_ref[:, pl.ds(at, wide)].astype(jnp.float32)
                hidden_ref[:, pl.ds(at, wide)] = old + row.astype(jnp.float32)

    hidden = hidden_ref[...]
    new_ref[...] = hidden.astype(new_ref.dtype)
    scale = lax.rsqrt(jnp.mean(hidden * hidden, axis=1, keepdims=True) + 1e-06)
    normed_ref[...] = (hidden * scale * gain_ref[...]).astype(normed_ref.dtype)


def finish(me, residual, gain, pieces):
    vmem = pl.BlockSpec(memory_space=pltpu.VMEM)
    out = jax.ShapeDtypeStruct(residual.shape, jnp.bfloat16)
    return pl.pallas_call(
        finish_kernel,
        in_specs=[pl.BlockSpec(memory_space=pltpu.SMEM)] + [vmem] * (2 + len(pieces)),
        out_specs=[vmem, vmem],
        out_shape=[out, out],
        scratch_shapes=[pltpu.VMEM(residual.shape, jnp.float32)],
        compiler_params=pltpu.CompilerParams(vmem_limit_bytes=8 * 1024 * 1024),
        name="finish",
    )(me, residual, gain, *pieces)


def per_device(
    q_nope, q_rope, latent, key_rope, absorb_key, absorb_value, w_out, residual, norm_gain, span_table
):
    f32, bf16 = jnp.float32, jnp.bfloat16
    tok, heads, size = q_nope.shape
    rope = q_rope.shape[2]
    n_seq, n_heads = lax.axis_size("seq"), lax.axis_size("heads")
    depth_z = n_seq // 4
    me = lax.axis_index("seq").astype(jnp.int32)
    core, slab = me & 1, me >> 2
    half = heads // 2

    line = depth_z == 4

    def swap(x, bit):
        return lax.ppermute(x, "seq", [(i, i ^ bit) for i in range(n_seq)])

    def move(x, pairs):
        return lax.ppermute(x, "seq", [(4 * a + r, 4 * b + r) for a, b in pairs for r in range(4)])

    kv_own = pack(latent, key_rope.T)
    zs, ys = [kv_own], [swap(kv_own, 2)]
    for k in range(1, depth_z):
        k = (k ^ (k >> 1)) if line else k
        zs.append(swap(kv_own, 4 * k))
        ys.append(swap(zs[-1], 2))
    if line:
        zs, ys = [zs[k] for k in (0, 1, 3, 2)], [ys[k] for k in (0, 1, 3, 2)]
    along, across = jnp.concatenate(zs, axis=0), jnp.concatenate(ys, axis=0)

    def split_heads(x, count):
        mine = lax.dynamic_slice_in_dim(x, core * count, count, 0)
        theirs = lax.dynamic_slice_in_dim(x, (1 - core) * count, count, 0)
        return mine, swap(theirs, 1)

    nope = split_heads(jnp.transpose(q_nope, (1, 0, 2)), half)
    rotary = split_heads(jnp.transpose(q_rope, (1, 2, 0)).reshape(heads * rope, tok), half * rope)

    wk = lax.dynamic_slice_in_dim(absorb_key, core * half, half, 0)
    wv = lax.dynamic_slice_in_dim(absorb_value, core * half, half, 0)
    head_group = lax.axis_index("heads").astype(jnp.int32).reshape(1)
    gain = norm_gain[None, :]
    along, head_group, gain, *own = lax.optimization_barrier(
        (along, head_group, gain, nope[0], rotary[0])
    )
    nope, rotary = (own[0], nope[1]), (own[1], rotary[1])
    parts = [along, across, swap(along, 1), swap(across, 1)]

    w_t = w_out.T
    cols = w_t.shape[0]
    span = half * size
    w_mine = lax.dynamic_slice_in_dim(w_t, core * span, span, 1)
    w_theirs = lax.dynamic_slice_in_dim(w_t, (1 - core) * span, span, 1)
    w_core = swap(w_theirs, 1)
    weights = [w_mine, w_core, swap(w_mine, 2), swap(w_core, 2)]

    groups = 2
    step_heads = max(
        h for h in (4, 2) if half // groups % h == 0 and h * tok * 8 * tok * depth_z <= 3 << 19
    )
    blocks = []
    for g in range(groups):
        mixed = attend(
            me.reshape(1),
            span_table,
            nope,
            rotary,
            parts,
            wk,
            wv,
            g,
            groups,
            step_heads,
        )
        if line:
            near, opposite = swap(mixed, 4), swap(mixed, 12)
            far = move(near, [(1, 2), (2, 1)])
            out = move(opposite, [(1, 0), (2, 3)])
            blocks.append([mixed, near, opposite, far, out])
        else:
            blocks.append([mixed] + [swap(mixed, 4 * k) for k in range(1, depth_z)])

    def reduce(keep, send):
        count = keep.shape[1]
        other = swap(send, 1)
        if n_heads == 2:
            mine, send = halve(head_group, keep, other)
            got = lax.ppermute(send, "heads", [(0, 1), (1, 0)])
            return list(join(mine, got))
        total = keep + jnp.stack([other[j ^ 1] for j in range(4)]).astype(f32)
        total = lax.psum_scatter(total.astype(bf16), "heads", scatter_dimension=2, tiled=True)
        return [total[:, n] for n in range(count)]

    if line:
        mixed, near, opposite, far, out = zip(*blocks)
        me1 = me.reshape(1)
        first = project(me1, [mixed, near], [], weights[:2], tok)
        early = project(me1, [mixed, near], [], weights, tok, first)
        middle = project(me1, [opposite], [], weights, tok)
        late = project(me1, [], [far, out], weights, tok)
        mine = reduce(*early) + reduce(*late) + reduce(*middle)
    else:
        rows = jnp.stack([jnp.concatenate(parts, axis=1) for parts in zip(*blocks)])
        total = jnp.einsum("zti,joi->jzto", rows, jnp.stack(weights), preferred_element_type=f32)
        mine = reduce(total[:, :, :tok], total[:, :, tok:].astype(bf16))
    pieces = [mine[0]] + [swap(mine[k], 4 * k) for k in range(1, depth_z)]
    if 4 * cols % 128 == 0:
        return tuple(finish(me.reshape(1), residual, gain, pieces))
    places = slab ^ jnp.arange(depth_z, dtype=jnp.int32)
    order = jnp.arange(depth_z, dtype=jnp.int32)
    order = jnp.sum(jnp.where(places[None, :] == order[:, None], order[None, :], 0), axis=1)
    columns = jnp.take(jnp.stack(pieces), order, axis=0)
    columns = jnp.take(columns, jnp.arange(4, dtype=jnp.int32) ^ (me & 3), axis=1)
    hidden = residual.astype(f32) + jnp.moveaxis(columns, 2, 0).reshape(residual.shape).astype(f32)
    scale = lax.rsqrt(jnp.mean(hidden * hidden, axis=1, keepdims=True) + 1e-06)
    return (hidden.astype(bf16), (hidden * scale * gain).astype(bf16))


def solution(mesh):
    in_specs = (
        P("seq", "heads", None),
        P("seq", "heads", None),
        P("seq", None),
        P("seq", None),
        P("heads", None, None),
        P("heads", None, None),
        P("heads", "seq"),
        P(("seq", "heads"), None),
        P(),
        P(),
    )
    out_specs = (P(("seq", "heads"), None), P(("seq", "heads"), None))

    return jax.shard_map(
        per_device, mesh=mesh, in_specs=in_specs, out_specs=out_specs, check_vma=False
    )
```
